32 devices in a mesh: keys: 8 (over z, y), view: 4 (over x, core).
Axes of the slice: x: 2, y: 2, z: 4, core: 2. Of those that a mesh axis runs over, the one named last changes fastest.
Arguments:
- key_slot: int32 [4096], replicated, may hold values from 0 to 4095, as said below
- a_slot: int32 [131072], P(('keys', 'view')), may hold values from 0 to 511
- a_group: int32 [131072], P(('keys', 'view')), may hold values from 0 to 1023
- a_weight: int32 [131072], P(('keys', 'view')), may hold values from 1 to 3
- a_payload: bfloat16 [131072, 256], P(('keys', 'view')), may hold values from -1.1953125 to 1.1953125
- b_slot: int32 [131072], P(('keys', 'view')), may hold values from 0 to 511
- b_weight: int32 [131072], P(('keys', 'view')), may hold values from 1 to 3
- b_payload: bfloat16 [131072, 256], P(('keys', 'view')), may hold values from -0.59765625 to 0.59765625
- da_key: int32 [32768], P(('keys', 'view')), may hold values from 0 to 4095, as said below
- da_group: int32 [32768], P(('keys', 'view')), may hold values from 0 to 1023
- da_mult: int32 [32768], P(('keys', 'view')), may hold values from -1 to 1, as said below
- da_payload: bfloat16 [32768, 256], P(('keys', 'view')), may hold values from -1.796875 to 1.796875
- da_count: int32 [32], P(('keys', 'view')), may hold values from 768 to 1024, as said below
- db_key: int32 [32768], P(('keys', 'view')), may hold values from 0 to 4095, as said below
- db_mult: int32 [32768], P(('keys', 'view')), may hold values from -1 to 1, as said below
- db_payload: bfloat16 [32768, 256], P(('keys', 'view')), may hold values from -1.1953125 to 1.1953125
- db_count: int32 [32], P(('keys', 'view')), may hold values from 768 to 1024, as said below
Outputs:
- view_delta: float32 [1024, 256], P(('keys', 'view'))
The draws below stay inside these ranges and needn't reach their ends.
Inputs may be any that keep to these rules, and one draw needn't show every extreme that they name: `key_slot`: A permutation of 0 to 4095. `da_key`: among the 1024 slots of one device, at most 256 have keys held by one keys index; in every draw one keys index gets exactly 256 live rows from every device. `db_key`: among the 1024 slots of one device, at most 256 have keys held by one keys index; in every draw one keys index gets exactly 256 live rows from every device. `da_mult`: each entry is -1 or 1. `db_mult`: each entry is -1 or 1. `da_count`: some device has all 1024 rows live. `db_count`: some device has all 1024 rows live.
All inputs are finite; a program needn't handle non-finite values.
Results may differ from the reference program's by a relative error of at most 0.0029.
Values may be sent and summed in bfloat16 or wider, within the bound.
A program may use at most 64 MiB of HBM per device.

```python
import jax
import jax.numpy as jnp

D = 256
KEYS_DEV = 512
GROUPS_DEV = 32
A_DEV = 4096
B_DEV = 4096
DELTA_DEV = 1024
CAP = 256
KEYS = 4096
GROUPS = 1024
A_ROWS = 131072
B_ROWS = 131072
DELTA_ROWS = 32768
N_KEYS = 8
N_VIEW = 4


def draw_key_slot(key, part):
    return jax.random.permutation(jax.random.fold_in(key, 11), KEYS).astype(jnp.int32)


def delta_keys(key, salt_value):
    order = draw_key_slot(key, 0)
    inverse = jnp.zeros((KEYS,), jnp.int32).at[order].set(jnp.arange(KEYS, dtype=jnp.int32))
    base = jax.random.fold_in(key, salt_value)
    hot_owner = jax.random.randint(jax.random.fold_in(base, 1), (), 0, N_KEYS).astype(jnp.int32)
    others = (hot_owner + 1 + jnp.arange(N_KEYS - 1, dtype=jnp.int32)) % N_KEYS
    target_pool = jnp.repeat(others, CAP, total_repeat_length=(N_KEYS - 1) * CAP)
    device_keys = jax.random.split(jax.random.fold_in(base, 2), N_KEYS * N_VIEW)

    def one_device(device_key):
        shuffled = jax.random.permutation(jax.random.fold_in(device_key, 3), target_pool)
        target = jnp.concatenate([jnp.full((CAP,), hot_owner, jnp.int32), shuffled[:DELTA_DEV - CAP]])
        within = jax.random.randint(jax.random.fold_in(device_key, 4), (DELTA_DEV,), 0, KEYS_DEV).astype(jnp.int32)
        return jnp.take(inverse, target * KEYS_DEV + within)
    return jax.vmap(one_device)(device_keys).reshape(-1).astype(jnp.int32)


def delta_signs(key, salt_value):
    picked = jax.random.randint(jax.random.fold_in(key, salt_value), (DELTA_ROWS,), 0, 2)
    return (2 * picked - 1).astype(jnp.int32)


def delta_counts(key, salt_value):
    devices = N_KEYS * N_VIEW
    counts = jax.random.randint(jax.random.fold_in(key, salt_value), (devices,), 3 * DELTA_DEV // 4, DELTA_DEV + 1)
    full_device = jax.random.randint(jax.random.fold_in(key, salt_value + 1), (), 0, devices)
    return counts.at[full_device].set(DELTA_DEV).astype(jnp.int32)


def draw_da_key(key, part):
    return delta_keys(key, 21)


def draw_db_key(key, part):
    return delta_keys(key, 22)


def draw_da_mult(key, part):
    return delta_signs(key, 31)


def draw_db_mult(key, part):
    return delta_signs(key, 32)


def draw_da_count(key, part):
    return delta_counts(key, 41)


def draw_db_count(key, part):
    return delta_counts(key, 51)


def plant(entries, own_key, smallest, high):
    dims = entries.shape
    place = [jax.random.randint(jax.random.fold_in(own_key, axis), (), 0, dims[axis]) for axis in range(len(dims))]
    entries = entries.at[tuple(place)].set(smallest)
    longest = dims.index(max(dims))
    place[longest] = (place[longest] + 1) % dims[longest]
    return entries.at[tuple(place)].set(high)


def block_scale(key, dims, pieces, least, high):
    gain = 1.0
    for axis_at, shards_of in pieces:
        heights = jax.random.uniform(jax.random.fold_in(jax.random.fold_in(key, 6), axis_at), (shards_of,), jnp.float32, least / len(pieces), high / len(pieces))
        gain = gain * jnp.repeat(jnp.exp(heights), dims[axis_at] // shards_of).reshape((-1,) + (1,) * (len(dims) - 1 - axis_at))
    return gain


def scatter_about(key, shape, width, bound, cuts=(), held_as=jnp.bfloat16):
    result = width * jax.random.normal(key, shape, jnp.float32)
    if cuts:
        result = result * block_scale(key, shape, cuts, -0.22, 0.18)
    return jnp.clip(result, -bound, bound).astype(held_as)


def setup_inputs(seed: int = 0) -> dict:
    splits = jax.random.split(jax.random.key(seed), 18)
    key_slot = draw_key_slot(jax.random.fold_in(splits[17], 71), 0)
    a_slot = plant(jax.random.randint(splits[1], (A_ROWS,), 0, KEYS_DEV), jax.random.fold_in(splits[1], 1), 0, KEYS_DEV - 1).astype(jnp.int32)
    a_group = plant(jax.random.randint(splits[2], (A_ROWS,), 0, GROUPS), jax.random.fold_in(splits[2], 1), 0, GROUPS - 1).astype(jnp.int32)
    a_weight = plant(jax.random.randint(splits[3], (A_ROWS,), 1, 4), jax.random.fold_in(splits[3], 1), 1, 3).astype(jnp.int32)
    a_payload = scatter_about(splits[4], (A_ROWS, D), 0.2, 1.1953125, ((0, 32),))
    b_slot = plant(jax.random.randint(splits[5], (B_ROWS,), 0, KEYS_DEV), jax.random.fold_in(splits[5], 1), 0, KEYS_DEV - 1).astype(jnp.int32)
    b_weight = plant(jax.random.randint(splits[6], (B_ROWS,), 1, 4), jax.random.fold_in(splits[6], 1), 1, 3).astype(jnp.int32)
    b_payload = scatter_about(splits[7], (B_ROWS, D), 0.1, 0.59765625, ((0, 32),))
    da_key = draw_da_key(jax.random.fold_in(splits[17], 71), 0)
    da_group = plant(jax.random.randint(splits[9], (DELTA_ROWS,), 0, GROUPS), jax.random.fold_in(splits[9], 1), 0, GROUPS - 1).astype(jnp.int32)
    da_mult = draw_da_mult(jax.random.fold_in(splits[17], 71), 0)
    da_payload = scatter_about(splits[11], (DELTA_ROWS, D), 0.3, 1.796875, ((0, 32),))
    da_count = draw_da_count(jax.random.fold_in(splits[17], 71), 0)
    db_key = draw_db_key(jax.random.fold_in(splits[17], 71), 0)
    db_mult = draw_db_mult(jax.random.fold_in(splits[17], 71), 0)
    db_payload = scatter_about(splits[15], (DELTA_ROWS, D), 0.2, 1.1953125, ((0, 32),))
    db_count = draw_db_count(jax.random.fold_in(splits[17], 71), 0)
    return dict(key_slot=key_slot, a_slot=a_slot, a_group=a_group, a_weight=a_weight, a_payload=a_payload, b_slot=b_slot, b_weight=b_weight, b_payload=b_payload, da_key=da_key, da_group=da_group, da_mult=da_mult, da_payload=da_payload, da_count=da_count, db_key=db_key, db_mult=db_mult, db_payload=db_payload, db_count=db_count)


def reference(key_slot, a_slot, a_group, a_weight, a_payload, b_slot, b_weight, b_payload, da_key, da_group, da_mult, da_payload, da_count, db_key, db_mult, db_payload, db_count):
    devices = N_KEYS * N_VIEW
    total_keys = KEYS_DEV * N_KEYS
    total_groups = GROUPS_DEV * devices

    def owner_slots(local_slot, rows_dev):
        device_index = jnp.arange(local_slot.shape[0], dtype=jnp.int32) // rows_dev
        return (device_index // N_VIEW) * KEYS_DEV + local_slot

    def signed_rows(row_mult, row_count):
        position = jnp.arange(DELTA_DEV * devices, dtype=jnp.int32)
        alive_rows = (position % DELTA_DEV) < jnp.take(row_count, position // DELTA_DEV)
        return (row_mult * alive_rows.astype(jnp.int32)).astype(jnp.float32)

    key_b = jax.ops.segment_sum(b_weight[:, None].astype(jnp.float32) * b_payload.astype(jnp.float32), owner_slots(b_slot, B_DEV), num_segments=total_keys)
    key_db = jax.ops.segment_sum(signed_rows(db_mult, db_count)[:, None] * db_payload.astype(jnp.float32), jnp.take(key_slot, db_key), num_segments=total_keys)
    a_terms = (a_weight[:, None].astype(jnp.float32) * a_payload.astype(jnp.float32) * jnp.take(key_db, owner_slots(a_slot, A_DEV), axis=0)).astype(jnp.bfloat16)
    whole_table = key_b + key_db
    delta_terms = (signed_rows(da_mult, da_count)[:, None] * da_payload.astype(jnp.float32) * jnp.take(whole_table, jnp.take(key_slot, da_key), axis=0)).astype(jnp.bfloat16)
    view_delta = jax.ops.segment_sum(a_terms.astype(jnp.float32), a_group, num_segments=total_groups)
    view_delta = view_delta + jax.ops.segment_sum(delta_terms.astype(jnp.float32), da_group, num_segments=total_groups)
    return view_delta
```

```python
import functools
import types

import jax
import jax.numpy as jnp
from jax import lax
from jax.experimental import pallas as pl
from jax.experimental.pallas import tpu as pltpu
from jax.sharding import PartitionSpec as P

LANES = 128
META = 8
F32 = jnp.float32
BF16 = jnp.bfloat16
VMEM_LIMIT = 62 * 1024 * 1024
MARKS_LIMIT = 16 * 1024 * 1024


def row_of(ref, start, count):
    return jnp.concatenate([ref[pl.ds(start + i, 1), :] for i in range(count)], axis=1)


def as_row(ref):
    return row_of(ref, 0, ref.shape[0])


def iota(shape, axis):
    return lax.broadcasted_iota(jnp.int32, shape, axis)


def dot(a, b):
    return jnp.dot(a, b, preferred_element_type=F32)


def hot(mask):
    return jnp.where(mask, 1.0, 0.0).astype(BF16)


def remote(src, dst, send, recv, keys, view):
    return pltpu.make_async_remote_copy(
        src_ref=src, dst_ref=dst, send_sem=send, recv_sem=recv,
        device_id=(keys, view), device_id_type=pl.DeviceIdType.MESH,
    )


def aligned(start, count):
    return pl.ds(pl.multiple_of(start, count), count)


def pack_plan(owners, keys_dev, cap, table_ref, key_ref, mult_ref, group_ref, count):
    key = as_row(key_ref)
    rows = key.shape[1]
    table = table_ref[...]
    tiles = table.shape[0]
    halves = jnp.concatenate([table & 255, table >> 8], axis=0).astype(F32).astype(BF16)
    looked = dot(halves, hot(iota((LANES, rows), 0) == (key & (LANES - 1))))
    high = iota((tiles, rows), 0) == (key >> 7)
    slot_low = jnp.sum(jnp.where(high, looked[:tiles], 0.0), axis=0, keepdims=True)
    slot_high = jnp.sum(jnp.where(high, looked[tiles:], 0.0), axis=0, keepdims=True)
    slot = slot_low.astype(jnp.int32) + 256 * slot_high.astype(jnp.int32)
    owner = slot // keys_dev
    local = slot - owner * keys_dev
    alive = iota((1, rows), 1) < count
    marks = jnp.where((iota((owners, rows), 0) == owner) & alive, 1.0, 0.0)
    step = min(256, rows)
    upper = hot(iota((step, step), 0) < iota((step, step), 1))
    running = jnp.zeros((owners, 1), F32)
    ranks = []
    for at in range(0, rows, step):
        piece = marks[:, at:at + step]
        before = dot(piece.astype(BF16), upper) + running
        ranks.append(jnp.sum(piece * before, axis=0, keepdims=True))
        running = running + jnp.sum(piece, axis=1, keepdims=True)
    rank = jnp.concatenate(ranks, axis=1).astype(jnp.int32)
    dest = jnp.where(alive, owner * cap + rank, -1)
    sign = as_row(mult_ref).astype(F32)
    parts = [local & 255, local >> 8]
    if group_ref is not None:
        group = as_row(group_ref)
        parts += [group & 255, group >> 8]
    meta = jnp.concatenate(
        [p.astype(F32) * sign for p in parts] + [jnp.zeros((META - len(parts), rows), F32)], axis=0
    ).astype(BF16)
    return dest, sign, meta


def packed(plan, cap, pay_ref, owner):
    dest, sign, meta = plan
    place = jnp.where(iota((cap, dest.shape[1]), 0) == dest - owner * cap, sign, 0.0).astype(BF16)
    columns = lax.dot_general(meta, place, (((1,), (1,)), ((), ())), preferred_element_type=F32)
    return dot(place, pay_ref[...]).astype(BF16), columns.astype(BF16)


def put_meta(ref, at, cap, columns):
    lanes = ref.shape[2]
    for t, lane in enumerate(range(0, cap, lanes)):
        wide = min(lanes, cap - lane)
        ref[at, cap + t * META:cap + (t + 1) * META, :wide] = columns[:, lane:lane + wide]


def meta_row(ref, at, row, cap):
    lanes = ref.shape[2]
    found = []
    for r in (row, row + 1):
        pieces = []
        for t, lane in enumerate(range(0, cap, lanes)):
            place = cap + t * META + r
            pieces.append(ref[at, place:place + 1, :min(lanes, cap - lane)].astype(F32))
        found.append(jnp.concatenate(pieces, axis=1).astype(jnp.int32))
    return found[0] + 256 * found[1]


def split(x):
    top = x.astype(BF16)
    return jnp.concatenate([top, (x - top.astype(F32)).astype(BF16)], axis=1)


def columns_of(row, width):
    return jnp.transpose(jnp.broadcast_to(row, (width, row.shape[1])))


def slot_marks(row, weight, keys_dev):
    count = row.shape[1]
    code = columns_of(row * 4 + weight, LANES)
    slot, scale = code >> 2, (code & 3).astype(F32)
    return jnp.concatenate(
        [
            jnp.where(iota((count, LANES), 1) + at == slot, scale, 0.0).astype(BF16)
            for at in range(0, keys_dev, LANES)
        ],
        axis=1,
    )


def kernel(d, *refs):
    (da_count, db_count, key_slot, a_slot, a_weight, a_group, b_slot, b_weight, da_key, da_group, da_mult,
     db_key, db_mult, a_hbm, b_hbm, da_hbm, db_hbm, out) = refs[:18]
    s = types.SimpleNamespace(**dict(zip(d.names, refs[18:], strict=True)))
    n, views, cap, slots, groups, width = d.owners, d.views, d.cap, d.slots, d.groups, d.width
    half, held = width // 2, d.held
    me, view = lax.axis_index("keys"), lax.axis_index("view")
    core = view & 1
    low = n // 2
    side = me // low
    place = me - side * low
    a_rows = s.a_pay.shape[0]

    loads = [
        pltpu.make_async_copy(src, dst, s.load.at[i])
        for i, (src, dst) in enumerate(
            ((db_hbm, s.db_pay), (da_hbm, s.da_pay), (b_hbm, s.b_pay), (a_hbm, s.a_pay))
        )
    ]
    for load in loads:
        load.start()

    barrier = pltpu.get_barrier_semaphore()
    devices = n * views
    mine = me * views + view

    def greet(i, carry):
        other = lax.rem(mine + i, devices)
        pl.semaphore_signal(
            barrier, inc=1, device_id=(other // views, lax.rem(other, views)),
            device_id_type=pl.DeviceIdType.MESH,
        )
        return carry

    lax.fori_loop(1, devices, greet, 0)

    b_plan = pack_plan(n, slots, cap, key_slot, db_key, db_mult, None, db_count[0])
    loads[0].wait()

    def b_pack(low_ref, high_ref, owner):
        rows, columns = packed(b_plan, cap, s.db_pay, owner)
        low_ref[owner, :cap, :] = rows[:, :half]
        high_ref[owner, :cap, :] = rows[:, half:]
        put_meta(low_ref, owner, cap, columns)

    def b_one(i, carry):
        b_pack(s.b_out0, s.b_out1, me ^ i)
        return carry

    lax.fori_loop(1, n, b_one, 0)
    b_pack(s.b_in0, s.b_in1, me)

    def b_copy(j, owner, source):
        src, dst = ((s.b_out0, s.b_in0), (s.b_out1, s.b_in1))[j]
        return remote(src.at[owner], dst.at[source], s.b_send.at[j, owner], s.b_recv.at[j, source], owner, view)

    pl.semaphore_wait(barrier, devices - 1)
    for j in range(2):
        def b_start(i, carry):
            b_copy(j, me ^ (n - i), me).start()
            return carry

        lax.fori_loop(1, n, b_start, 0)

    d_plan = pack_plan(n, slots, cap, key_slot, da_key, da_mult, da_group, da_count[0])
    loads[1].wait()
    from_me = core * low + place

    def d_pack(ref, at, owner):
        rows, columns = packed(d_plan, cap, s.da_pay, owner)
        ref[at, :cap, :] = rows
        put_meta(ref, at, cap, columns)

    def d_copy(owner, source):
        there = owner // low
        return remote(
            s.d_out.at[owner], s.d_in.at[source], s.d_send.at[owner], s.d_recv.at[source],
            side * low + owner - there * low, (view - core) + there,
        )

    def d_one(i, carry):
        owner = from_me ^ (n - i)
        d_pack(s.d_out, owner, owner)
        d_copy(owner, from_me).start()
        return carry

    lax.fori_loop(1, n, d_one, 0)
    d_pack(s.d_in, from_me, from_me)

    def total_steps(part, first, mids, lasts, total, send, recv):
        cut = slots // 2
        keep, give = aligned(core * cut, cut), aligned((1 - core) * cut, cut)
        bits = [1 << b for b in range(1, views.bit_length() - 1)]

        def copy(i):
            if i == 0:
                return remote(part.at[give], first, send.at[0], recv.at[0], me, view ^ 1)
            if i <= len(bits):
                return remote(mids.at[i - 1], lasts.at[i - 1], send.at[i], recv.at[i], me, view ^ bits[i - 1])
            return remote(total.at[keep], total.at[keep], send.at[i], recv.at[i], me, view ^ 1)

        def arrived(i):
            copy(i).wait_recv()
            return part[keep, :] + first[...] if i == 0 else mids[i - 1] + lasts[i - 1]

        def step(i):
            def run():
                if i > len(bits) + 1:
                    copy(i - 1).wait_recv()
                    return
                if 0 < i <= len(bits):
                    mids[i - 1] = arrived(i - 1)
                if i == len(bits) + 1:
                    total[keep, :] = arrived(i - 1)
                copy(i).start()
            return run

        count = len(bits) + 2
        return [step(i) for i in range(count + 1)], [copy(i) for i in range(count)]

    base_steps, base_sent = total_steps(
        s.base, s.base_first, s.base_mid, s.base_last, s.base_total, s.base_send, s.base_recv
    )
    halves = [
        total_steps(
            s.part.at[j], s.part_first.at[j], s.part_mid.at[j], s.part_last.at[j], s.part_total.at[j],
            s.part_send.at[j], s.part_recv.at[j],
        )
        for j in range(2)
    ]

    loads[2].wait()
    chunk = min(1024, s.b_pay.shape[0])
    lines = chunk // LANES
    s.base[...] = jnp.zeros_like(s.base)

    def base_one(c, carry):
        slot = row_of(b_slot, c * lines, lines)
        weight = row_of(b_weight, c * lines, lines).astype(F32)
        marks = jnp.where(iota((slots, chunk), 0) == slot, weight, 0.0).astype(BF16)
        s.base[...] += dot(marks, s.b_pay[aligned(c * chunk, chunk), :])
        return carry

    lax.fori_loop(0, s.b_pay.shape[0] // chunk, base_one, 0)
    base_steps[0]()

    few = min(256, a_rows)
    few_lines = few // LANES

    def slot_one(c, carry):
        s.a_marks[aligned(c * few, few), :] = slot_marks(
            row_of(a_slot, c * few_lines, few_lines), row_of(a_weight, c * few_lines, few_lines), slots
        )
        return carry

    lax.fori_loop(0, a_rows // few, slot_one, 0)
    base_steps[1]()

    block = min(256, groups // 2)
    blocks = groups // 2 // block
    span = min(1024, a_rows)
    span_lines = span // LANES

    def group_ids(g):
        second = g // blocks
        at = iota((block, 1), 0) + (g - second * blocks) * block
        to = at // held
        bit = jnp.where(second == 0, 1 - core, core)
        return (to * 2 + bit) * held + (at - to * held)

    def a_group_marks(g, c):
        return hot(group_ids(g) == row_of(a_group, c * span_lines, span_lines))

    if d.keep:
        def group_one(g, carry):
            for c in range(a_rows // span):
                s.a_groups[aligned(g * block, block), c * span:(c + 1) * span] = a_group_marks(g, c)
            return carry

        lax.fori_loop(0, blocks, group_one, 0)
    for step in base_steps[2:-1]:
        step()
    if d.keep:
        lax.fori_loop(blocks, 2 * blocks, group_one, 0)
    base_steps[-1]()

    def delta_sum(j):
        arrived_at = (s.b_in0, s.b_in1)[j]
        part = s.part.at[j]

        def one(source):
            if j == 0:
                s.b_marks[source] = hot(iota((slots, cap), 0) == meta_row(s.b_in0, source, 0, cap))
            return dot(s.b_marks[source], arrived_at[source, :cap, :])

        part[...] = one(me)

        def step(i, carry):
            source = me ^ (n - i)
            b_copy(j, source, source).wait_recv()
            part[...] += one(source)
            return carry

        lax.fori_loop(1, n, step, 0)

    def a_gather(j):
        s.a_table[...] = split(s.part_total[j])
        lanes = slice(j * half, (j + 1) * half)

        def step(c, carry):
            rows = aligned(c * few, few)
            both = dot(s.a_marks[rows, :], s.a_table[...])
            s.a_terms[rows, lanes] = (
                s.a_pay[rows, lanes].astype(F32) * (both[:, :half] + both[:, half:])
            ).astype(BF16)
            return carry

        lax.fori_loop(0, a_rows // few, step, 0)

    def table_copy(j):
        return remote(s.d_table.at[j], s.d_table.at[j], s.t_send.at[j], s.t_recv.at[j], me ^ low, view)

    def table_send(j):
        @pl.when(core == side)
        def _():
            s.d_table[j] = split(s.part_total[j] + s.base_total[:, j * half:(j + 1) * half])
            table_copy(j).start()

    def d_arrive():
        def one(source):
            s.d_marks[source] = slot_marks(meta_row(s.d_in, source, 0, cap), jnp.ones((1, cap), jnp.int32), slots)
            group = meta_row(s.d_in, source, 2, cap)
            if d.keep:
                def fill(g, carry):
                    s.d_groups[source, aligned(g * block, block), :] = hot(group_ids(g) == group)
                    return carry

                lax.fori_loop(0, 2 * blocks, fill, 0)

        one(from_me)

        def step(i, carry):
            source = from_me ^ (n - i)
            d_copy(source, source).wait_recv()
            one(source)
            return carry

        lax.fori_loop(1, n, step, 0)

    delta_sum(0)
    steps = halves[0][0]
    steps[0]()
    loads[3].wait()
    for step in steps[1:]:
        step()
    table_send(0)
    a_gather(0)
    delta_sum(1)
    steps = halves[1][0]
    steps[0]()
    steps[1]()
    d_arrive()
    for step in steps[2:]:
        step()
    table_send(1)
    a_gather(1)

    def a_sum(g, carry):
        rows = aligned(g * block, block)
        if d.keep:
            s.view[rows, :] = dot(s.a_groups[rows, :], s.a_terms[...])
        else:
            s.view[rows, :] = sum(
                dot(a_group_marks(g, c), s.a_terms[c * span:(c + 1) * span, :]) for c in range(a_rows // span)
            )
        return carry

    lax.fori_loop(0, 2 * blocks, a_sum, 0)

    @pl.when(core != side)
    def _():
        for j in range(2):
            table_copy(j).wait_recv()

    def d_gather(source, carry):
        for j in range(2):
            lanes = slice(j * half, (j + 1) * half)
            both = dot(s.d_marks[source], s.d_table[j])
            s.d_terms[source, :, lanes] = (
                s.d_in[source, :cap, lanes].astype(F32) * (both[:, :half] + both[:, half:])
            ).astype(BF16)
        return carry

    lax.fori_loop(0, n, d_gather, 0)

    def d_sum(g):
        rows = aligned(g * block, block)
        ids = group_ids(g)

        def one(source, total):
            if d.keep:
                marks = s.d_groups[source, rows, :]
            else:
                marks = hot(ids == meta_row(s.d_in, source, 2, cap))
            return total + dot(marks, s.d_terms[source])

        return lax.fori_loop(0, n, one, s.view[rows, :])

    def pair_copy(g):
        rows = aligned(g * block, block)
        return remote(s.give.at[rows], s.take.at[rows], s.p_send.at[g], s.p_recv.at[g], me, view ^ 1)

    def give_one(g, carry):
        s.give[aligned(g * block, block), :] = d_sum(g)
        pair_copy(g).start()
        return carry

    lax.fori_loop(0, blocks, give_one, 0)
    pairs = views // 2
    spot = me * pairs + view // 2
    per = block // held

    def piece_copy(to, source):
        owner = to // pairs
        return remote(
            s.pieces.at[to], s.inbox.at[source], s.o_send.at[to], s.o_recv.at[source],
            owner, (to - owner * pairs) * 2 + core,
        )

    def keep_one(g, carry):
        total = d_sum(g + blocks)
        pair_copy(g).wait_recv()
        total = (total + s.take[aligned(g * block, block), :]).astype(BF16)
        for i in range(per):
            s.pieces[g * per + i] = total[i * held:(i + 1) * held, :]

        def send(i, inner):
            to = g * per + i

            @pl.when(to != spot)
            def _():
                piece_copy(to, spot).start()
            return inner

        lax.fori_loop(0, per, send, 0)
        return carry

    lax.fori_loop(0, blocks, keep_one, 0)
    out[...] = s.pieces[spot].astype(F32)
    everyone = n * pairs

    def collect(i, carry):
        source = lax.rem(spot + i, everyone)
        piece_copy(source, source).wait_recv()
        out[...] += s.inbox[source].astype(F32)
        return carry

    lax.fori_loop(1, everyone, collect, 0)

    def finish(i, carry):
        for j in range(2):
            b_copy(j, me ^ i, me).wait_send()
        d_copy(from_me ^ i, from_me).wait_send()
        return carry

    lax.fori_loop(1, n, finish, 0)
    for sent in base_sent + halves[0][1] + halves[1][1]:
        sent.wait_send()

    @pl.when(core == side)
    def _():
        for j in range(2):
            table_copy(j).wait_send()

    def pair_done(g, carry):
        pair_copy(g).wait_send()
        return carry

    lax.fori_loop(0, blocks, pair_done, 0)

    def piece_done(i, carry):
        piece_copy(lax.rem(spot + i, everyone), spot).wait_send()
        return carry

    lax.fori_loop(1, everyone, piece_done, 0)


def shards(
    groups, key_slot, a_slot, a_group, a_weight, a_payload, b_slot, b_weight, b_payload,
    da_key, da_group, da_mult, da_payload, da_count, db_key, db_mult, db_payload, db_count,
):
    owners, views = lax.axis_size("keys"), lax.axis_size("view")
    a_rows, width = a_payload.shape
    slots = key_slot.shape[0] // owners
    delta = da_payload.shape[0]
    cap = 2 * delta // owners
    half = width // 2
    held = groups // (owners * views)
    bits = max(1, views.bit_length() - 2)
    block = min(256, groups // 2)
    blocks = groups // 2 // block
    keep = 2 * groups * (a_rows + owners * cap) <= MARKS_LIMIT

    def lined(x):
        return x.reshape(-1, LANES)

    def tail(lanes):
        return max(2 * META, META * -(-cap // lanes))

    cut = slots // 2
    dma = pltpu.SemaphoreType.DMA
    scratch = dict(
        a_pay=pltpu.VMEM(a_payload.shape, BF16),
        b_pay=pltpu.VMEM(b_payload.shape, BF16),
        da_pay=pltpu.VMEM(da_payload.shape, BF16),
        db_pay=pltpu.VMEM(db_payload.shape, BF16),
        b_out0=pltpu.VMEM((owners, cap + tail(half), half), BF16),
        b_out1=pltpu.VMEM((owners, cap, half), BF16),
        b_in0=pltpu.VMEM((owners, cap + tail(half), half), BF16),
        b_in1=pltpu.VMEM((owners, cap, half), BF16),
        d_out=pltpu.VMEM((owners, cap + tail(width), width), BF16),
        d_in=pltpu.VMEM((owners, cap + tail(width), width), BF16),
        b_marks=pltpu.VMEM((owners, slots, cap), BF16),
        a_marks=pltpu.VMEM((a_rows, slots), BF16),
        d_marks=pltpu.VMEM((owners, cap, slots), BF16),
        base=pltpu.VMEM((slots, width), F32),
        base_first=pltpu.VMEM((cut, width), F32),
        base_mid=pltpu.VMEM((bits, cut, width), F32),
        base_last=pltpu.VMEM((bits, cut, width), F32),
        base_total=pltpu.VMEM((slots, width), F32),
        part=pltpu.VMEM((2, slots, half), F32),
        part_first=pltpu.VMEM((2, cut, half), F32),
        part_mid=pltpu.VMEM((2, bits, cut, half), F32),
        part_last=pltpu.VMEM((2, bits, cut, half), F32),
        part_total=pltpu.VMEM((2, slots, half), F32),
        a_table=pltpu.VMEM((slots, width), BF16),
        d_table=pltpu.VMEM((2, slots, width), BF16),
        a_terms=pltpu.VMEM((a_rows, width), BF16),
        d_terms=pltpu.VMEM((owners, cap, width), BF16),
        view=pltpu.VMEM((groups, width), F32),
        give=pltpu.VMEM((groups // 2, width), F32),
        take=pltpu.VMEM((groups // 2, width), F32),
        pieces=pltpu.VMEM((owners * views // 2, held, width), BF16),
        inbox=pltpu.VMEM((owners * views // 2, held, width), BF16),
        load=dma((4,)),
        b_send=dma((2, owners)),
        b_recv=dma((2, owners)),
        d_send=dma((owners,)),
        d_recv=dma((owners,)),
        base_send=dma((bits + 2,)),
        base_recv=dma((bits + 2,)),
        part_send=dma((2, bits + 2)),
        part_recv=dma((2, bits + 2)),
        t_send=dma((2,)),
        t_recv=dma((2,)),
        p_send=dma((blocks,)),
        p_recv=dma((blocks,)),
        o_send=dma((owners * views // 2,)),
        o_recv=dma((owners * views // 2,)),
    )
    if keep:
        scratch["a_groups"] = pltpu.VMEM((groups, a_rows), BF16)
        scratch["d_groups"] = pltpu.VMEM((owners, groups, cap), BF16)
    dims = types.SimpleNamespace(
        names=tuple(scratch), owners=owners, views=views, cap=cap, slots=slots, groups=groups, width=width,
        held=held, keep=keep,
    )
    vmem, smem = pl.BlockSpec(memory_space=pltpu.VMEM), pl.BlockSpec(memory_space=pltpu.SMEM)
    away = pl.BlockSpec(memory_space=pl.ANY)
    return pl.pallas_call(
        functools.partial(kernel, dims),
        out_shape=jax.ShapeDtypeStruct((held, width), F32),
        in_specs=[smem] * 2 + [vmem] * 11 + [away] * 4,
        out_specs=vmem,
        scratch_shapes=list(scratch.values()),
        compiler_params=pltpu.CompilerParams(
            collective_id=0, has_side_effects=True, vmem_limit_bytes=VMEM_LIMIT
        ),
        name="delta_view",
    )(
        da_count, db_count, lined(key_slot), lined(a_slot), lined(a_weight), lined(a_group), lined(b_slot),
        lined(b_weight), lined(da_key), lined(da_group), lined(da_mult), lined(db_key), lined(db_mult),
        a_payload, b_payload, da_payload, db_payload,
    )


GROUPS_DEV = 32


def solution(mesh):
    row, wide = P(("keys", "view")), P(("keys", "view"), None)
    groups = GROUPS_DEV * mesh.shape["keys"] * mesh.shape["view"]
    in_specs = (P(), row, row, row, wide, row, row, wide, row, row, row, wide, row, row, row, wide, row)
    return jax.shard_map(
        functools.partial(shards, groups), mesh=mesh, in_specs=in_specs, out_specs=wide, check_vma=False
    )
```

```python
import functools
import types

import jax
import jax.numpy as jnp
from jax import lax
from jax.experimental import pallas as pl
from jax.experimental.pallas import tpu as pltpu
from jax.sharding import PartitionSpec as P

LANES = 128
META = 8
F32 = jnp.float32
BF16 = jnp.bfloat16
VMEM_LIMIT = 62 * 1024 * 1024
MARKS_LIMIT = 16 * 1024 * 1024


def row_of(ref, start, count):
    return jnp.concatenate([ref[pl.ds(start + i, 1), :] for i in range(count)], axis=1)


def as_row(ref):
    return row_of(ref, 0, ref.shape[0])


def iota(shape, axis):
    return lax.broadcasted_iota(jnp.int32, shape, axis)


def dot(a, b):
    return jnp.dot(a, b, preferred_element_type=F32)


def hot(mask):
    return jnp.where(mask, 1.0, 0.0).astype(BF16)


def remote(src, dst, send, recv, keys, view):
    return pltpu.make_async_remote_copy(
        src_ref=src, dst_ref=dst, send_sem=send, recv_sem=recv,
        device_id=(keys, view), device_id_type=pl.DeviceIdType.MESH,
    )


def aligned(start, count):
    return pl.ds(pl.multiple_of(start, count), count)


def pack_plan(owners, keys_dev, cap, table_ref, key_ref, mult_ref, group_ref, count):
    key = as_row(key_ref)
    rows = key.shape[1]
    table = table_ref[...]
    tiles = table.shape[0]
    halves = jnp.concatenate([table & 255, table >> 8], axis=0).astype(F32).astype(BF16)
    looked = dot(halves, hot(iota((LANES, rows), 0) == (key & (LANES - 1))))
    high = iota((tiles, rows), 0) == (key >> 7)
    slot_low = jnp.sum(jnp.where(high, looked[:tiles], 0.0), axis=0, keepdims=True)
    slot_high = jnp.sum(jnp.where(high, looked[tiles:], 0.0), axis=0, keepdims=True)
    slot = slot_low.astype(jnp.int32) + 256 * slot_high.astype(jnp.int32)
    owner = slot // keys_dev
    local = slot - owner * keys_dev
    alive = iota((1, rows), 1) < count
    marks = jnp.where((iota((owners, rows), 0) == owner) & alive, 1.0, 0.0)
    step = min(256, rows)
    upper = hot(iota((step, step), 0) < iota((step, step), 1))
    running = jnp.zeros((owners, 1), F32)
    ranks = []
    for at in range(0, rows, step):
        piece = marks[:, at:at + step]
        before = dot(piece.astype(BF16), upper) + running
        ranks.append(jnp.sum(piece * before, axis=0, keepdims=True))
        running = running + jnp.sum(piece, axis=1, keepdims=True)
    rank = jnp.concatenate(ranks, axis=1).astype(jnp.int32)
    dest = jnp.where(alive, owner * cap + rank, -1)
    sign = as_row(mult_ref).astype(F32)
    parts = [local & 255, local >> 8]
    if group_ref is not None:
        group = as_row(group_ref)
        parts += [group & 255, group >> 8]
    meta = jnp.concatenate(
        [p.astype(F32) * sign for p in parts] + [jnp.zeros((META - len(parts), rows), F32)], axis=0
    ).astype(BF16)
    return dest, sign, meta


def packed(plan, cap, pay_ref, owner):
    dest, sign, meta = plan
    place = jnp.where(iota((cap, dest.shape[1]), 0) == dest - owner * cap, sign, 0.0).astype(BF16)
    columns = lax.dot_general(meta, place, (((1,), (1,)), ((), ())), preferred_element_type=F32)
    return dot(place, pay_ref[...]).astype(BF16), columns.astype(BF16)


def put_meta(ref, at, cap, columns):
    lanes = ref.shape[2]
    for t, lane in enumerate(range(0, cap, lanes)):
        wide = min(lanes, cap - lane)
        ref[at, cap + t * META:cap + (t + 1) * META, :wide] = columns[:, lane:lane + wide]


def meta_row(ref, at, row, cap):
    lanes = ref.shape[2]
    found = []
    for r in (row, row + 1):
        pieces = []
        for t, lane in enumerate(range(0, cap, lanes)):
            place = cap + t * META + r
            pieces.append(ref[at, place:place + 1, :min(lanes, cap - lane)].astype(F32))
        found.append(jnp.concatenate(pieces, axis=1).astype(jnp.int32))
    return found[0] + 256 * found[1]


def split(x):
    top = x.astype(BF16)
    return jnp.concatenate([top, (x - top.astype(F32)).astype(BF16)], axis=1)


def columns_of(row, width):
    return jnp.transpose(jnp.broadcast_to(row, (width, row.shape[1])))


def slot_marks(row, weight, keys_dev):
    count = row.shape[1]
    code = columns_of(row * 4 + weight, LANES)
    slot, scale = code >> 2, (code & 3).astype(F32)
    return jnp.concatenate(
        [
            jnp.where(iota((count, LANES), 1) + at == slot, scale, 0.0).astype(BF16)
            for at in range(0, keys_dev, LANES)
        ],
        axis=1,
    )


def kernel(d, *refs):
    (da_count, db_count, key_slot, a_slot, a_weight, a_group, b_slot, b_weight, da_key, da_group, da_mult,
     db_key, db_mult, a_hbm, b_hbm, da_hbm, db_hbm, out) = refs[:18]
    s = types.SimpleNamespace(**dict(zip(d.names, refs[18:], strict=True)))
    n, views, cap, slots, groups, width = d.owners, d.views, d.cap, d.slots, d.groups, d.width
    half, held = width // 2, d.held
    me, view = lax.axis_index("keys"), lax.axis_index("view")
    core = view & 1
    low = n // 2
    side = me // low
    place = me - side * low
    a_rows = s.a_pay.shape[0]

    loads = [
        pltpu.make_async_copy(src, dst, s.load.at[i])
        for i, (src, dst) in enumerate(
            ((db_hbm, s.db_pay), (da_hbm, s.da_pay), (b_hbm, s.b_pay), (a_hbm, s.a_pay))
        )
    ]
    for load in loads:
        load.start()

    barrier = pltpu.get_barrier_semaphore()
    devices = n * views
    mine = me * views + view

    def greet(i, carry):
        other = lax.rem(mine + i, devices)
        pl.semaphore_signal(
            barrier, inc=1, device_id=(other // views, lax.rem(other, views)),
            device_id_type=pl.DeviceIdType.MESH,
        )
        return carry

    lax.fori_loop(1, devices, greet, 0)

    b_plan = pack_plan(n, slots, cap, key_slot, db_key, db_mult, None, db_count[0])
    loads[0].wait()

    from_me = core * low + place

    def row_copy(src, dst, send, recv, owner, source):
        there = owner // low
        return remote(
            src.at[owner], dst.at[source], send.at[owner], recv.at[source],
            side * low + owner - there * low, (view - core) + there,
        )

    def b_copy(j, owner, source):
        src, dst = ((s.b_out0, s.b_in0), (s.b_out1, s.b_in1))[j]
        return row_copy(src, dst, s.b_send.at[j], s.b_recv.at[j], owner, source)

    def d_copy(owner, source):
        return row_copy(s.d_out, s.d_in, s.d_send, s.d_recv, owner, source)

    def b_pack(low_ref, high_ref, at):
        rows, columns = packed(b_plan, cap, s.db_pay, at)
        low_ref[at, :cap, :] = rows[:, :half]
        high_ref[at, :cap, :] = rows[:, half:]
        put_meta(low_ref, at, cap, columns)

    def b_one(i, carry):
        b_pack(s.b_out0, s.b_out1, from_me ^ (n - i))
        return carry

    def b_start(j, i, carry):
        b_copy(j, from_me ^ (n - i), from_me).start()
        return carry

    def b_both(i, carry):
        b_one(i, carry)
        return b_start(0, i, carry)

    early = min(4, n)
    lax.fori_loop(1, early, b_one, 0)
    pl.semaphore_wait(barrier, devices - 1)
    lax.fori_loop(1, early, functools.partial(b_start, 0), 0)
    lax.fori_loop(early, n, b_both, 0)
    lax.fori_loop(1, n, functools.partial(b_start, 1), 0)
    b_pack(s.b_in0, s.b_in1, from_me)

    d_plan = pack_plan(n, slots, cap, key_slot, da_key, da_mult, da_group, da_count[0])
    loads[1].wait()
    def d_pack(ref, at, owner):
        rows, columns = packed(d_plan, cap, s.da_pay, owner)
        ref[at, :cap, :] = rows
        put_meta(ref, at, cap, columns)

    step_z = max(1, low // 2)

    def d_fill(i, carry):
        owner = from_me ^ i
        d_pack(s.d_out, owner, owner)
        return carry

    def d_start(i, carry):
        near = lax.rem(i, step_z)
        owner = from_me ^ ((i - near) * 2 + step_z + near)
        d_copy(owner, from_me).start()
        return carry

    def d_near(i, carry):
        near = lax.rem(i, step_z)
        owner = from_me ^ ((i - near) * 2 + near)
        d_copy(owner, from_me).start()
        return carry

    lax.fori_loop(1, n, d_fill, 0)
    lax.fori_loop(1, n // 2, d_near, 0)
    d_pack(s.d_in, from_me, from_me)

    @pl.when(core == side)
    def _():
        lax.fori_loop(0, n // 2, d_start, 0)

    right = core == side
    wide = views // 2
    spot_x = view // 2
    piece = slots // wide
    own = aligned(spot_x * piece, piece)
    peers = [lax.rem(spot_x + i, wide) for i in range(1, wide)]

    def wrong(run):
        pl.when(core != side)(run)

    base_pair = remote(s.base, s.base_first, s.pair_send, s.pair_recv, me, view ^ 1)

    def base_copy(p, source):
        at = aligned(p * piece, piece)
        return remote(s.base.at[at], s.base_in.at[source], s.base_send.at[p], s.base_recv.at[source], me, p * 2 + core)

    def base_add():
        @pl.when(right)
        def _():
            base_pair.wait_recv()
            s.base[...] += s.base_first[...]
            for p in peers:
                base_copy(p, spot_x).start()

    def base_end():
        @pl.when(right)
        def _():
            s.base_total[...] = s.base[own, :]
            for p in peers:
                base_copy(p, p).wait_recv()
                s.base_total[...] += s.base_in[p]

    def wide_copy(j, p, source):
        at = aligned(p * piece, piece)
        return remote(
            s.part.at[j, at], s.part_in.at[j, source], s.w_send.at[j, p], s.w_recv.at[j, source], me, p * 2 + core
        )

    def cross_copy(j):
        return remote(s.part_mid.at[j], s.part_first.at[j], s.x_send.at[j], s.x_recv.at[j], me ^ low, view)

    def total_copy(j, i, source):
        at = s.part_total.at[j, aligned(source * piece, piece)]
        return remote(at, at, s.g_send.at[j, i], s.g_recv.at[j, source], me, lax.rem(view + i, views))

    def table_copy(j, source):
        at = s.d_table.at[j, aligned(source * piece, piece)]
        return remote(at, at, s.c_send.at[j], s.t_recv.at[j, source], me ^ low, view)

    def table_peer(j, p, source):
        at = s.d_table.at[j, aligned(source * piece, piece)]
        return remote(at, at, s.t_send.at[j, p], s.t_recv.at[j, source], me, p * 2 + core)

    def wide_give(j):
        for p in peers:
            wide_copy(j, p, spot_x).start()

    def wide_take(j):
        s.part_mid[j] = s.part[j, own]
        for p in peers:
            wide_copy(j, p, p).wait_recv()
            s.part_mid[j] += s.part_in[j, p]
        wrong(lambda: cross_copy(j).start())

    def total_give(j):
        @pl.when(right)
        def _():
            cross_copy(j).wait_recv()
            total = s.part_mid[j] + s.part_first[j]
            s.part_total[j, own] = total
            for i in range(1, views):
                total_copy(j, i, spot_x).start()
            s.d_table[j, own] = split(total + s.base_total[:, j * half:(j + 1) * half])
            table_copy(j, spot_x).start()
            for p in peers:
                table_peer(j, p, spot_x).start()

    def total_take(j):
        for p in peers:
            total_copy(j, 0, p).wait_recv()
        wrong(lambda: total_copy(j, 0, spot_x).wait_recv())

    def table_relay(j):
        @wrong
        def _():
            table_copy(j, spot_x).wait_recv()
            for p in peers:
                table_peer(j, p, spot_x).start()

    def table_take(j):
        for p in peers:
            table_peer(j, p, p).wait_recv()

    loads[2].wait()
    chunk = min(1024, s.b_pay.shape[0])
    lines = chunk // LANES
    s.base[...] = jnp.zeros_like(s.base)

    def base_one(c, carry):
        slot = row_of(b_slot, c * lines, lines)
        weight = row_of(b_weight, c * lines, lines).astype(F32)
        marks = jnp.where(iota((slots, chunk), 0) == slot, weight, 0.0).astype(BF16)
        s.base[...] += dot(marks, s.b_pay[aligned(c * chunk, chunk), :])
        return carry

    lax.fori_loop(0, s.b_pay.shape[0] // chunk, base_one, 0)
    wrong(base_pair.start)

    few = min(512, a_rows)
    few_lines = few // LANES

    def slot_one(c, carry):
        s.a_marks[aligned(c * few, few), :] = slot_marks(
            row_of(a_slot, c * few_lines, few_lines), row_of(a_weight, c * few_lines, few_lines), slots
        )
        return carry

    block = min(256, groups // 2)
    blocks = groups // 2 // block
    span = min(1024, a_rows)
    span_lines = span // LANES

    def group_place(group):
        to = group // held
        return (to >> 1) * held + group - to * held + jnp.where((to & 1) == core, groups // 2, 0)

    s.a_place[...] = group_place(a_group[...])

    def group_marks(g, count, at):
        return hot(iota((count, at.shape[1]), 0) + g * count == at)

    def a_group_marks(g, c):
        return group_marks(g, block, row_of(s.a_place, c * span_lines, span_lines))

    def a_groups():
        if not d.keep:
            return

        def one(g, carry):
            for c in range(a_rows // span):
                s.a_groups[aligned(g * block, block), c * span:(c + 1) * span] = a_group_marks(g, c)
            return carry

        lax.fori_loop(0, 2 * blocks, one, 0)

    def delta_sum(j):
        arrived_at = (s.b_in0, s.b_in1)[j]

        def fill(source):
            if j == 0:
                marks = hot(iota((slots, cap), 0) == meta_row(s.b_in0, source, 0, cap))
                if d.flat:
                    s.b_marks[:, aligned(source * cap, cap)] = marks
                else:
                    s.b_marks[source] = marks

        fill(from_me)

        def step(i, carry):
            source = from_me ^ (n - i)
            b_copy(j, source, source).wait_recv()
            fill(source)
            return carry

        lax.fori_loop(1, n, step, 0)
        if d.flat:
            s.part[j] = dot(s.b_marks[...], arrived_at[:, :cap, :].reshape(n * cap, half))
        else:
            s.part[j] = lax.fori_loop(
                0, n, lambda i, total: total + dot(s.b_marks[i], arrived_at[i, :cap, :]), jnp.zeros((slots, half), F32)
            )

    def a_gather(j):
        s.a_table[...] = split(s.part_total[j])
        lanes = slice(j * half, (j + 1) * half)

        def step(c, carry):
            rows = aligned(c * span, span)
            both = dot(s.a_marks[rows, :], s.a_table[...])
            s.a_terms[rows, lanes] = (
                s.a_pay[rows, lanes].astype(F32) * (both[:, :half] + both[:, half:])
            ).astype(BF16)
            return carry

        lax.fori_loop(0, a_rows // span, step, 0)

    def d_arrive():
        def one(source):
            rows = aligned(source * cap, cap)
            s.d_marks[rows, :] = slot_marks(meta_row(s.d_in, source, 0, cap), jnp.ones((1, cap), jnp.int32), slots)
            if d.keep:
                s.d_groups[:, rows] = group_marks(0, groups, group_place(meta_row(s.d_in, source, 2, cap)))

        one(from_me)

        def step(i, carry):
            source = from_me ^ (n - i)
            d_copy(source, source).wait_recv()
            one(source)
            return carry

        lax.fori_loop(1, n, step, 0)

    delta_sum(0)
    wide_give(0)
    base_add()
    lax.fori_loop(0, a_rows // few, slot_one, 0)

    a_groups()
    wide_take(0)
    delta_sum(1)
    wide_give(1)
    base_end()
    loads[3].wait()
    wide_take(1)
    @wrong
    def _():
        lax.fori_loop(0, n // 2, d_start, 0)

    total_give(0)
    total_take(0)
    a_gather(0)
    total_give(1)
    table_relay(0)
    d_arrive()
    total_take(1)
    a_gather(1)
    table_relay(1)

    def a_sum(g, carry):
        rows = aligned(g * block, block)
        if d.keep:
            s.view[rows, :] = dot(s.a_groups[rows, :], s.a_terms[...])
        else:
            s.view[rows, :] = sum(
                dot(a_group_marks(g, c), s.a_terms[c * span:(c + 1) * span, :]) for c in range(a_rows // span)
            )
        return carry

    lax.fori_loop(0, 2 * blocks, a_sum, 0)

    for j in range(2):
        table_take(j)

    several = min(n, span // cap)

    def d_gather(c, carry):
        rows = aligned(c * several * cap, several * cap)
        for j in range(2):
            lanes = slice(j * half, (j + 1) * half)
            both = dot(s.d_marks[rows, :], s.d_table[j])
            pay = s.d_in[pl.ds(c * several, several), :cap, lanes].reshape(several * cap, half)
            s.d_terms[rows, lanes] = (pay.astype(F32) * (both[:, :half] + both[:, half:])).astype(BF16)
        return carry

    lax.fori_loop(0, n // several, d_gather, 0)

    def d_sum(g):
        rows = aligned(g * block, block)
        if d.keep:
            return s.view[rows, :] + dot(s.d_groups[rows, :], s.d_terms[...])

        def one(source, total):
            marks = group_marks(g, block, group_place(meta_row(s.d_in, source, 2, cap)))
            return total + dot(marks, s.d_terms[aligned(source * cap, cap), :])

        return lax.fori_loop(0, n, one, s.view[rows, :])

    def pair_copy(g):
        rows = aligned(g * block, block)
        return remote(s.give.at[rows], s.take.at[rows], s.p_send.at[g], s.p_recv.at[g], me, view ^ 1)

    def give_one(g, carry):
        s.give[aligned(g * block, block), :] = d_sum(g)
        pair_copy(g).start()
        return carry

    lax.fori_loop(0, blocks, give_one, 0)
    pairs = views // 2
    spot = me * pairs + view // 2
    per = block // held

    def piece_copy(to, source):
        owner = to // pairs
        return remote(
            s.pieces.at[to], s.inbox.at[source], s.o_send.at[to], s.o_recv.at[source],
            owner, (to - owner * pairs) * 2 + core,
        )

    def keep_one(g, carry):
        total = d_sum(g + blocks)
        pair_copy(g).wait_recv()
        total = (total + s.take[aligned(g * block, block), :]).astype(BF16)
        for i in range(per):
            s.pieces[g * per + i] = total[i * held:(i + 1) * held, :]

        def send(i, inner):
            to = g * per + i

            @pl.when(to != spot)
            def _():
                piece_copy(to, spot).start()
            return inner

        lax.fori_loop(0, per, send, 0)
        return carry

    lax.fori_loop(0, blocks, keep_one, 0)
    out[...] = s.pieces[spot].astype(F32)
    everyone = n * pairs

    def collect(i, carry):
        source = lax.rem(spot + i, everyone)
        piece_copy(source, source).wait_recv()
        out[...] += s.inbox[source].astype(F32)
        return carry

    lax.fori_loop(1, everyone, collect, 0)

    def finish(i, carry):
        for j in range(2):
            b_copy(j, from_me ^ i, from_me).wait_send()
        d_copy(from_me ^ i, from_me).wait_send()
        return carry

    lax.fori_loop(1, n, finish, 0)

    @wrong
    def _():
        base_pair.wait_send()
        for j in range(2):
            cross_copy(j).wait_send()

    @pl.when(right)
    def _():
        for p in peers:
            base_copy(p, spot_x).wait_send()
        for j in range(2):
            for i in range(1, views):
                total_copy(j, i, spot_x).wait_send()
            table_copy(j, spot_x).wait_send()

    for j in range(2):
        for p in peers:
            wide_copy(j, p, spot_x).wait_send()
            table_peer(j, p, spot_x).wait_send()

    def pair_done(g, carry):
        pair_copy(g).wait_send()
        return carry

    lax.fori_loop(0, blocks, pair_done, 0)

    def piece_done(i, carry):
        piece_copy(lax.rem(spot + i, everyone), spot).wait_send()
        return carry

    lax.fori_loop(1, everyone, piece_done, 0)


def shards(
    groups, key_slot, a_slot, a_group, a_weight, a_payload, b_slot, b_weight, b_payload,
    da_key, da_group, da_mult, da_payload, da_count, db_key, db_mult, db_payload, db_count,
):
    owners, views = lax.axis_size("keys"), lax.axis_size("view")
    a_rows, width = a_payload.shape
    slots = key_slot.shape[0] // owners
    delta = da_payload.shape[0]
    cap = 2 * delta // owners
    half = width // 2
    held = groups // (owners * views)
    wide = views // 2
    piece = slots // wide
    block = min(256, groups // 2)
    blocks = groups // 2 // block
    flat = cap % LANES == 0
    keep = flat and 2 * groups * (a_rows + owners * cap) <= MARKS_LIMIT

    def lined(x):
        return x.reshape(-1, LANES)

    def tail(lanes):
        return max(2 * META, META * -(-cap // lanes))

    dma = pltpu.SemaphoreType.DMA
    scratch = dict(
        a_pay=pltpu.VMEM(a_payload.shape, BF16),
        b_pay=pltpu.VMEM(b_payload.shape, BF16),
        da_pay=pltpu.VMEM(da_payload.shape, BF16),
        db_pay=pltpu.VMEM(db_payload.shape, BF16),
        b_out0=pltpu.VMEM((owners, cap + tail(half), half), BF16),
        b_out1=pltpu.VMEM((owners, cap, half), BF16),
        b_in0=pltpu.VMEM((owners, cap + tail(half), half), BF16),
        b_in1=pltpu.VMEM((owners, cap, half), BF16),
        d_out=pltpu.VMEM((owners, cap + tail(width), width), BF16),
        d_in=pltpu.VMEM((owners, cap + tail(width), width), BF16),
        b_marks=pltpu.VMEM((slots, owners * cap) if flat else (owners, slots, cap), BF16),
        a_marks=pltpu.VMEM((a_rows, slots), BF16),
        d_marks=pltpu.VMEM((owners * cap, slots), BF16),
        base=pltpu.VMEM((slots, width), F32),
        base_first=pltpu.VMEM((slots, width), F32),
        base_in=pltpu.VMEM((wide, piece, width), F32),
        base_total=pltpu.VMEM((piece, width), F32),
        part=pltpu.VMEM((2, slots, half), F32),
        part_in=pltpu.VMEM((2, wide, piece, half), F32),
        part_mid=pltpu.VMEM((2, piece, half), F32),
        part_first=pltpu.VMEM((2, piece, half), F32),
        part_total=pltpu.VMEM((2, slots, half), F32),
        a_table=pltpu.VMEM((slots, width), BF16),
        d_table=pltpu.VMEM((2, slots, width), BF16),
        a_terms=pltpu.VMEM((a_rows, width), BF16),
        d_terms=pltpu.VMEM((owners * cap, width), BF16),
        a_place=pltpu.VMEM((a_rows // LANES, LANES), jnp.int32),
        view=pltpu.VMEM((groups, width), F32),
        give=pltpu.VMEM((groups // 2, width), F32),
        take=pltpu.VMEM((groups // 2, width), F32),
        pieces=pltpu.VMEM((owners * views // 2, held, width), BF16),
        inbox=pltpu.VMEM((owners * views // 2, held, width), BF16),
        load=dma((4,)),
        b_send=dma((2, owners)),
        b_recv=dma((2, owners)),
        d_send=dma((owners,)),
        d_recv=dma((owners,)),
        pair_send=dma,
        pair_recv=dma,
        base_send=dma((wide,)),
        base_recv=dma((wide,)),
        w_send=dma((2, wide)),
        w_recv=dma((2, wide)),
        x_send=dma((2,)),
        x_recv=dma((2,)),
        g_send=dma((2, views)),
        g_recv=dma((2, wide)),
        c_send=dma((2,)),
        t_send=dma((2, wide)),
        t_recv=dma((2, wide)),
        p_send=dma((blocks,)),
        p_recv=dma((blocks,)),
        o_send=dma((owners * views // 2,)),
        o_recv=dma((owners * views // 2,)),
    )
    if keep:
        scratch["a_groups"] = pltpu.VMEM((groups, a_rows), BF16)
        scratch["d_groups"] = pltpu.VMEM((groups, owners * cap), BF16)
    dims = types.SimpleNamespace(
        names=tuple(scratch), owners=owners, views=views, cap=cap, slots=slots, groups=groups, width=width,
        held=held, keep=keep, flat=flat,
    )
    vmem, smem = pl.BlockSpec(memory_space=pltpu.VMEM), pl.BlockSpec(memory_space=pltpu.SMEM)
    away = pl.BlockSpec(memory_space=pl.ANY)
    return pl.pallas_call(
        functools.partial(kernel, dims),
        out_shape=jax.ShapeDtypeStruct((held, width), F32),
        in_specs=[smem] * 2 + [vmem] * 11 + [away] * 4,
        out_specs=vmem,
        scratch_shapes=list(scratch.values()),
        compiler_params=pltpu.CompilerParams(
            collective_id=0, has_side_effects=True, vmem_limit_bytes=VMEM_LIMIT
        ),
        name="delta_view",
    )(
        da_count, db_count, lined(key_slot), lined(a_slot), lined(a_weight), lined(a_group), lined(b_slot),
        lined(b_weight), lined(da_key), lined(da_group), lined(da_mult), lined(db_key), lined(db_mult),
        a_payload, b_payload, da_payload, db_payload,
    )


GROUPS_DEV = 32


def solution(mesh):
    row, wide = P(("keys", "view")), P(("keys", "view"), None)
    groups = GROUPS_DEV * mesh.shape["keys"] * mesh.shape["view"]
    in_specs = (P(), row, row, row, wide, row, row, wide, row, row, row, wide, row, row, row, wide, row)
    return jax.shard_map(
        functools.partial(shards, groups), mesh=mesh, in_specs=in_specs, out_specs=wide, check_vma=False
    )
```

```python
import functools
import types

import jax
import jax.numpy as jnp
from jax import lax
from jax.experimental import pallas as pl
from jax.experimental.pallas import tpu as pltpu
from jax.sharding import PartitionSpec as P

LANES = 128
META = 8
F32 = jnp.float32
BF16 = jnp.bfloat16
VMEM_LIMIT = 62 * 1024 * 1024
MARKS_LIMIT = 16 * 1024 * 1024


def row_of(ref, start, count):
    return jnp.concatenate([ref[pl.ds(start + i, 1), :] for i in range(count)], axis=1)


def as_row(ref):
    return row_of(ref, 0, ref.shape[0])


def iota(shape, axis):
    return lax.broadcasted_iota(jnp.int32, shape, axis)


def dot(a, b):
    return jnp.dot(a, b, preferred_element_type=F32)


def hot(mask):
    return jnp.where(mask, 1.0, 0.0).astype(BF16)


def remote(src, dst, send, recv, keys, view):
    return pltpu.make_async_remote_copy(
        src_ref=src, dst_ref=dst, send_sem=send, recv_sem=recv,
        device_id=(keys, view), device_id_type=pl.DeviceIdType.MESH,
    )


def aligned(start, count):
    return pl.ds(pl.multiple_of(start, count), count)


def pack_plan(owners, keys_dev, cap, table_ref, key_ref, mult_ref, group_ref, count):
    key = as_row(key_ref)
    rows = key.shape[1]
    table = table_ref[...]
    tiles = table.shape[0]
    halves = jnp.concatenate([table & 255, table >> 8], axis=0).astype(F32).astype(BF16)
    looked = dot(halves, hot(iota((LANES, rows), 0) == (key & (LANES - 1))))
    high = iota((tiles, rows), 0) == (key >> 7)
    slot_low = jnp.sum(jnp.where(high, looked[:tiles], 0.0), axis=0, keepdims=True)
    slot_high = jnp.sum(jnp.where(high, looked[tiles:], 0.0), axis=0, keepdims=True)
    slot = slot_low.astype(jnp.int32) + 256 * slot_high.astype(jnp.int32)
    owner = slot // keys_dev
    local = slot - owner * keys_dev
    alive = iota((1, rows), 1) < count
    marks = jnp.where((iota((owners, rows), 0) == owner) & alive, 1.0, 0.0)
    step = min(256, rows)
    upper = hot(iota((step, step), 0) < iota((step, step), 1))
    running = jnp.zeros((owners, 1), F32)
    ranks = []
    for at in range(0, rows, step):
        piece = marks[:, at:at + step]
        before = dot(piece.astype(BF16), upper) + running
        ranks.append(jnp.sum(piece * before, axis=0, keepdims=True))
        running = running + jnp.sum(piece, axis=1, keepdims=True)
    rank = jnp.concatenate(ranks, axis=1).astype(jnp.int32)
    dest = jnp.where(alive, owner * cap + rank, -1)
    sign = as_row(mult_ref).astype(F32)
    parts = [local & 255, local >> 8]
    if group_ref is not None:
        group = as_row(group_ref)
        parts += [group & 255, group >> 8]
    meta = jnp.concatenate(
        [p.astype(F32) * sign for p in parts] + [jnp.zeros((META - len(parts), rows), F32)], axis=0
    ).astype(BF16)
    return dest, sign, meta


def packed(plan, cap, pay_ref, owner):
    dest, sign, meta = plan
    place = jnp.where(iota((cap, dest.shape[1]), 0) == dest - owner * cap, sign, 0.0).astype(BF16)
    columns = lax.dot_general(meta, place, (((1,), (1,)), ((), ())), preferred_element_type=F32)
    return dot(place, pay_ref[...]).astype(BF16), columns.astype(BF16)


def put_meta(ref, at, cap, columns):
    lanes = ref.shape[2]
    for t, lane in enumerate(range(0, cap, lanes)):
        wide = min(lanes, cap - lane)
        ref[at, cap + t * META:cap + (t + 1) * META, :wide] = columns[:, lane:lane + wide]


def meta_row(ref, at, row, cap):
    lanes = ref.shape[2]
    found = []
    for r in (row, row + 1):
        pieces = []
        for t, lane in enumerate(range(0, cap, lanes)):
            place = cap + t * META + r
            pieces.append(ref[at, place:place + 1, :min(lanes, cap - lane)].astype(F32))
        found.append(jnp.concatenate(pieces, axis=1).astype(jnp.int32))
    return found[0] + 256 * found[1]


def split(x):
    top = x.astype(BF16)
    return jnp.concatenate([top, (x - top.astype(F32)).astype(BF16)], axis=1)


def columns_of(row, width):
    return jnp.transpose(jnp.broadcast_to(row, (width, row.shape[1])))


def slot_marks(row, weight, keys_dev):
    count = row.shape[1]
    code = columns_of(row * 4 + weight, LANES)
    slot, scale = code >> 2, (code & 3).astype(F32)
    return jnp.concatenate(
        [
            jnp.where(iota((count, LANES), 1) + at == slot, scale, 0.0).astype(BF16)
            for at in range(0, keys_dev, LANES)
        ],
        axis=1,
    )


def kernel(d, *refs):
    (da_count, db_count, key_slot, a_slot, a_weight, a_group, b_slot, b_weight, da_key, da_group, da_mult,
     db_key, db_mult, a_hbm, b_hbm, da_hbm, db_hbm, out) = refs[:18]
    s = types.SimpleNamespace(**dict(zip(d.names, refs[18:], strict=True)))
    n, views, cap, slots, groups, width = d.owners, d.views, d.cap, d.slots, d.groups, d.width
    half, held = width // 2, d.held
    me, view = lax.axis_index("keys"), lax.axis_index("view")
    core = view & 1
    low = n // 2
    side = me // low
    place = me - side * low
    a_rows = s.a_pay.shape[0]

    loads = [
        pltpu.make_async_copy(src, dst, s.load.at[i])
        for i, (src, dst) in enumerate(
            ((db_hbm, s.db_pay), (da_hbm, s.da_pay), (b_hbm, s.b_pay), (a_hbm, s.a_pay))
        )
    ]
    for load in loads:
        load.start()

    barrier = pltpu.get_barrier_semaphore()
    devices = n * views
    mine = me * views + view

    def greet(i, carry):
        other = lax.rem(mine + i, devices)
        pl.semaphore_signal(
            barrier, inc=1, device_id=(other // views, lax.rem(other, views)),
            device_id_type=pl.DeviceIdType.MESH,
        )
        return carry

    lax.fori_loop(1, devices, greet, 0)

    b_plan = pack_plan(n, slots, cap, key_slot, db_key, db_mult, None, db_count[0])
    loads[0].wait()

    from_me = core * low + place

    def row_copy(src, dst, send, recv, owner, source):
        there = owner // low
        return remote(
            src.at[owner], dst.at[source], send.at[owner], recv.at[source],
            side * low + owner - there * low, (view - core) + there,
        )

    def b_copy(j, owner, source):
        src, dst = ((s.b_out0, s.b_in0), (s.b_out1, s.b_in1))[j]
        return row_copy(src, dst, s.b_send.at[j], s.b_recv.at[j], owner, source)

    def d_copy(owner, source):
        return row_copy(s.d_out, s.d_in, s.d_send, s.d_recv, owner, source)

    def b_pack(low_ref, high_ref, at):
        rows, columns = packed(b_plan, cap, s.db_pay, at)
        low_ref[at, :cap, :] = rows[:, :half]
        high_ref[at, :cap, :] = rows[:, half:]
        put_meta(low_ref, at, cap, columns)

    def b_one(i, carry):
        b_pack(s.b_out0, s.b_out1, from_me ^ (n - i))
        return carry

    def b_start(j, i, carry):
        b_copy(j, from_me ^ (n - i), from_me).start()
        return carry

    def b_both(i, carry):
        b_one(i, carry)
        return b_start(0, i, carry)

    early = min(3, n)
    lax.fori_loop(1, early, b_one, 0)
    pl.semaphore_wait(barrier, devices - 1)
    lax.fori_loop(1, early, functools.partial(b_start, 0), 0)
    lax.fori_loop(early, n, b_both, 0)
    lax.fori_loop(1, n, functools.partial(b_start, 1), 0)
    b_pack(s.b_in0, s.b_in1, from_me)

    right = core == side
    wide = views // 2
    spot_x = view // 2
    piece = slots // wide
    own = aligned(spot_x * piece, piece)
    peers = [lax.rem(spot_x + i, wide) for i in range(1, wide)]

    def wrong(run):
        pl.when(core != side)(run)

    base_pair = remote(s.base, s.base_first, s.pair_send, s.pair_recv, me, view ^ 1)

    def base_copy(p, source):
        at = aligned(p * piece, piece)
        return remote(s.base.at[at], s.base_in.at[source], s.base_send.at[p], s.base_recv.at[source], me, p * 2 + core)

    def base_add():
        @pl.when(right)
        def _():
            base_pair.wait_recv()
            s.base[...] += s.base_first[...]
            for p in peers:
                base_copy(p, spot_x).start()

    def base_end():
        @pl.when(right)
        def _():
            s.base_total[own, :] = s.base[own, :]
            for p in peers:
                base_copy(p, p).wait_recv()
                s.base_total[own, :] += s.base_in[p]

    def base_all(p, source):
        at = s.base_total.at[aligned(source * piece, piece)]
        return remote(at, at, s.all_send.at[p], s.all_recv.at[source], me, p * 2 + core)

    def base_spread():
        @pl.when(right)
        def _():
            for p in peers:
                base_all(p, spot_x).start()

    sub = piece // 2
    subs = [pl.ds(q * sub, sub) for q in range(2)]

    def part_of(p, q):
        return aligned(p * piece + q * sub, sub)

    def wide_copy(j, p, source, q):
        return remote(
            s.part.at[j, part_of(p, q)], s.part_in.at[j, source, subs[q]],
            s.w_send.at[j, p, q], s.w_recv.at[j, source, q], me, p * 2 + core,
        )

    def cross_copy(j, q):
        return remote(
            s.part_mid.at[j, subs[q]], s.part_first.at[j, subs[q]], s.x_send.at[j, q], s.x_recv.at[j, q], me ^ low, view
        )

    def total_copy(j, i, source, q):
        at = s.part_total.at[j, part_of(source, q)]
        return remote(at, at, s.g_send.at[j, i, q], s.g_recv.at[j, source, q], me, lax.rem(view + i, views))

    def table_copy(j, source, q):
        at = s.d_table.at[j, part_of(source, q)]
        return remote(at, at, s.c_send.at[j, q], s.t_recv.at[j, source, q], me ^ low, view)

    def table_peer(j, p, source, q):
        at = s.d_table.at[j, part_of(source, q)]
        return remote(at, at, s.t_send.at[j, p, q], s.t_recv.at[j, source, q], me, p * 2 + core)

    def wide_give(j):
        for q in range(2):
            for p in peers:
                wide_copy(j, p, spot_x, q).start()

    def wide_take(j):
        for q in range(2):
            total = s.part[j, part_of(spot_x, q)]
            for p in peers:
                wide_copy(j, p, p, q).wait_recv()
                total += s.part_in[j, p, subs[q]]
            s.part_mid[j, subs[q]] = total
            wrong(lambda: cross_copy(j, q).start())

    def total_give(j):
        @pl.when(right)
        def _():
            for q in range(2):
                cross_copy(j, q).wait_recv()
                total = s.part_mid[j, subs[q]] + s.part_first[j, subs[q]]
                s.part_total[j, part_of(spot_x, q)] = total
                for i in range(1, views):
                    total_copy(j, i, spot_x, q).start()

    def table_give(j):
        @pl.when(right)
        def _():
            for q in range(2):
                at = part_of(spot_x, q)
                s.d_table[j, at] = split(s.part_total[j, at] + s.base_total[at, j * half:(j + 1) * half])
                table_copy(j, spot_x, q).start()

    def total_take(j):
        for q in range(2):
            for p in peers:
                total_copy(j, 0, p, q).wait_recv()
            wrong(lambda: total_copy(j, 0, spot_x, q).wait_recv())

    def table_relay(j):
        @wrong
        def _():
            for q in range(2):
                table_copy(j, spot_x, q).wait_recv()
                for p in peers:
                    table_peer(j, p, spot_x, q).start()

    def table_take(j):
        @wrong
        def _():
            for q in range(2):
                for p in peers:
                    table_peer(j, p, p, q).wait_recv()

        @pl.when(right)
        def _():
            for p in peers:
                at = aligned(p * piece, piece)
                s.d_table[j, at] = split(s.part_total[j, at] + s.base_total[at, j * half:(j + 1) * half])

    loads[2].wait()
    chunk = min(1024, s.b_pay.shape[0])
    lines = chunk // LANES
    s.base[...] = jnp.zeros_like(s.base)

    def base_one(c, carry):
        slot = row_of(b_slot, c * lines, lines)
        weight = row_of(b_weight, c * lines, lines).astype(F32)
        marks = jnp.where(iota((slots, chunk), 0) == slot, weight, 0.0).astype(BF16)
        s.base[...] += dot(marks, s.b_pay[aligned(c * chunk, chunk), :])
        return carry

    lax.fori_loop(0, s.b_pay.shape[0] // chunk, base_one, 0)
    wrong(base_pair.start)

    few = min(512, a_rows)
    few_lines = few // LANES

    def slot_one(c, carry):
        s.a_marks[aligned(c * few, few), :] = slot_marks(
            row_of(a_slot, c * few_lines, few_lines), row_of(a_weight, c * few_lines, few_lines), slots
        )
        return carry

    d_plan = pack_plan(n, slots, cap, key_slot, da_key, da_mult, da_group, da_count[0])
    loads[1].wait()
    def d_pack(ref, at, owner):
        rows, columns = packed(d_plan, cap, s.da_pay, owner)
        ref[at, :cap, :] = rows
        put_meta(ref, at, cap, columns)

    step_z = max(1, low // 2)

    def d_fill(i, carry):
        owner = from_me ^ i
        d_pack(s.d_out, owner, owner)
        return carry

    def d_start(i, carry):
        near = lax.rem(i, step_z)
        owner = from_me ^ ((i - near) * 2 + step_z + near)
        d_copy(owner, from_me).start()
        return carry

    def d_near(i, carry):
        near = lax.rem(i, step_z)
        owner = from_me ^ ((i - near) * 2 + near)
        d_copy(owner, from_me).start()
        return carry

    lax.fori_loop(1, n, d_fill, 0)
    lax.fori_loop(1, n // 2, d_near, 0)
    d_pack(s.d_in, from_me, from_me)

    @pl.when(core == side)
    def _():
        lax.fori_loop(0, n // 2, d_start, 0)

    block = min(256, groups // 2)
    blocks = groups // 2 // block
    span = min(2048, a_rows)
    span_lines = span // LANES

    def group_place(group):
        to = group // held
        turned = (to >> 1) ^ ((1 - side) * (devices // 4))
        return turned * held + group - to * held + jnp.where((to & 1) == core, groups // 2, 0)

    s.a_place[...] = group_place(a_group[...])

    def group_marks(g, count, at):
        return hot(iota((count, at.shape[1]), 0) + g * count == at)

    def a_group_marks(g, c):
        return group_marks(g, block, row_of(s.a_place, c * span_lines, span_lines))

    def a_groups():
        if not d.keep:
            return

        def one(g, carry):
            for c in range(a_rows // span):
                s.a_groups[aligned(g * block, block), c * span:(c + 1) * span] = a_group_marks(g, c)
            return carry

        lax.fori_loop(0, 2 * blocks, one, 0)

    def delta_sum(j):
        arrived_at = (s.b_in0, s.b_in1)[j]

        def fill(source):
            if j == 0:
                marks = hot(iota((slots, cap), 0) == meta_row(s.b_in0, source, 0, cap))
                if d.flat:
                    s.b_marks[:, aligned(source * cap, cap)] = marks
                else:
                    s.b_marks[source] = marks

        def step(i, carry):
            source = from_me ^ (n - i)
            b_copy(j, source, source).wait_recv()
            fill(source)
            return carry

        def gather(of):
            first = of * low
            rows = arrived_at[pl.ds(first, low), :cap, :].reshape(low * cap, half)
            if d.flat:
                return dot(s.b_marks[:, aligned(first * cap, low * cap)], rows)
            return lax.fori_loop(
                first, first + low, lambda i, total: total + dot(s.b_marks[i], arrived_at[i, :cap, :]),
                jnp.zeros((slots, half), F32),
            )

        lax.fori_loop(1, n - low + 1, step, 0)
        s.part[j] = gather(1 - core)
        fill(from_me)
        lax.fori_loop(n - low + 1, n, step, 0)
        s.part[j] += gather(core)

    def a_gather(j):
        s.a_table[...] = split(s.part_total[j])
        lanes = slice(j * half, (j + 1) * half)

        def step(c, carry):
            rows = aligned(c * span, span)
            both = dot(s.a_marks[rows, :], s.a_table[...])
            s.a_terms[rows, lanes] = (
                s.a_pay[rows, lanes].astype(F32) * (both[:, :half] + both[:, half:])
            ).astype(BF16)
            return carry

        lax.fori_loop(0, a_rows // span, step, 0)

    def d_arrive(first, last, far):
        def one(source):
            rows = aligned(source * cap, cap)
            s.d_marks[rows, :] = slot_marks(meta_row(s.d_in, source, 0, cap), jnp.ones((1, cap), jnp.int32), slots)
            if d.keep:
                s.d_groups[:, rows] = group_marks(0, groups, group_place(meta_row(s.d_in, source, 2, cap)))

        if first == 0 and not far:
            one(from_me)

        def step(i, carry):
            if far:
                i = lax.rem(i + jnp.where(core == side, 0, n // 4), n // 2)
            near = lax.rem(i, step_z)
            source = from_me ^ ((i - near) * 2 + near + (step_z if far else 0))
            d_copy(source, source).wait_recv()
            one(source)
            return carry

        lax.fori_loop(first if far else max(first, 1), last, step, 0)

    def a_sum(first, last):
        def step(g, carry):
            rows = aligned(g * block, block)
            if d.keep:
                s.view[rows, :] = dot(s.a_groups[rows, :], s.a_terms[...])
            else:
                s.view[rows, :] = sum(
                    dot(a_group_marks(g, c), s.a_terms[c * span:(c + 1) * span, :]) for c in range(a_rows // span)
                )
            return carry

        lax.fori_loop(first, last, step, 0)

    base_add()
    delta_sum(0)
    wide_give(0)
    lax.fori_loop(0, a_rows // few, slot_one, 0)

    delta_sum(1)
    wide_give(1)
    wide_take(0)
    a_groups()
    base_end()
    loads[3].wait()
    wide_take(1)
    @wrong
    def _():
        lax.fori_loop(0, n // 2, d_start, 0)

    total_give(0)
    total_give(1)
    table_give(0)
    table_give(1)
    base_spread()
    d_arrive(0, n // 2, False)
    total_take(0)
    a_gather(0)
    total_take(1)
    table_relay(0)
    a_gather(1)
    a_sum(0, blocks)
    table_relay(1)
    a_sum(blocks, 2 * blocks)
    d_arrive(0, n // 2, True)

    @pl.when(right)
    def _():
        for p in peers:
            base_all(p, p).wait_recv()

    for j in range(2):
        table_take(j)

    several = min(n, span // cap)

    def d_gather(c, carry):
        rows = aligned(c * several * cap, several * cap)
        for j in range(2):
            lanes = slice(j * half, (j + 1) * half)
            both = dot(s.d_marks[rows, :], s.d_table[j])
            pay = s.d_in[pl.ds(c * several, several), :cap, lanes].reshape(several * cap, half)
            s.d_terms[rows, lanes] = (pay.astype(F32) * (both[:, :half] + both[:, half:])).astype(BF16)
        return carry

    lax.fori_loop(0, n // several, d_gather, 0)

    def d_sum(g):
        rows = aligned(g * block, block)
        if d.keep:
            return s.view[rows, :] + dot(s.d_groups[rows, :], s.d_terms[...])

        def one(source, total):
            marks = group_marks(g, block, group_place(meta_row(s.d_in, source, 2, cap)))
            return total + dot(marks, s.d_terms[aligned(source * cap, cap), :])

        return lax.fori_loop(0, n, one, s.view[rows, :])

    def pair_copy(g):
        rows = aligned(g * block, block)
        return remote(s.give.at[rows], s.take.at[rows], s.p_send.at[g], s.p_recv.at[g], me, view ^ 1)

    def give_one(g, carry):
        s.give[aligned(g * block, block), :] = d_sum(g)
        pair_copy(g).start()
        return carry

    lax.fori_loop(0, blocks, give_one, 0)
    pairs = views // 2
    spot = me * pairs + view // 2
    per = block // held

    def piece_copy(to, source):
        owner = to // pairs
        return remote(
            s.pieces.at[to], s.inbox.at[source], s.o_send.at[to], s.o_recv.at[source],
            owner, (to - owner * pairs) * 2 + core,
        )

    def keep_one(g, carry):
        total = d_sum(g + blocks)
        pair_copy(g).wait_recv()
        total = (total + s.take[aligned(g * block, block), :]).astype(BF16)
        for i in range(per):
            s.pieces[(g * per + i) ^ ((1 - side) * (devices // 4))] = total[i * held:(i + 1) * held, :]

        def send(i, inner):
            to = (g * per + i) ^ ((1 - side) * (devices // 4))

            @pl.when(to != spot)
            def _():
                piece_copy(to, spot).start()
            return inner

        lax.fori_loop(0, per, send, 0)
        return carry

    lax.fori_loop(0, blocks, keep_one, 0)
    everyone = n * pairs
    out[0] = s.pieces[spot].astype(F32)
    out[1] = jnp.zeros(out.shape[1:], F32)

    def collect(i, carry):
        source = lax.rem(spot + i, everyone)
        piece_copy(source, source).wait_recv()
        at = i & 1
        out[at] += s.inbox[source].astype(F32)
        return carry

    lax.fori_loop(1, everyone, collect, 0)

    def finish(i, carry):
        for j in range(2):
            b_copy(j, from_me ^ i, from_me).wait_send()
        d_copy(from_me ^ i, from_me).wait_send()
        return carry

    lax.fori_loop(1, n, finish, 0)

    @wrong
    def _():
        base_pair.wait_send()
        for j in range(2):
            for q in range(2):
                cross_copy(j, q).wait_send()
                for p in peers:
                    table_peer(j, p, spot_x, q).wait_send()

    @pl.when(right)
    def _():
        for p in peers:
            base_copy(p, spot_x).wait_send()
            base_all(p, spot_x).wait_send()
        for j in range(2):
            for q in range(2):
                for i in range(1, views):
                    total_copy(j, i, spot_x, q).wait_send()
                table_copy(j, spot_x, q).wait_send()

    for j in range(2):
        for q in range(2):
            for p in peers:
                wide_copy(j, p, spot_x, q).wait_send()

    def pair_done(g, carry):
        pair_copy(g).wait_send()
        return carry

    lax.fori_loop(0, blocks, pair_done, 0)

    def piece_done(i, carry):
        piece_copy(lax.rem(spot + i, everyone), spot).wait_send()
        return carry

    lax.fori_loop(1, everyone, piece_done, 0)


def shards(
    groups, key_slot, a_slot, a_group, a_weight, a_payload, b_slot, b_weight, b_payload,
    da_key, da_group, da_mult, da_payload, da_count, db_key, db_mult, db_payload, db_count,
):
    owners, views = lax.axis_size("keys"), lax.axis_size("view")
    a_rows, width = a_payload.shape
    slots = key_slot.shape[0] // owners
    delta = da_payload.shape[0]
    cap = 2 * delta // owners
    half = width // 2
    held = groups // (owners * views)
    wide = views // 2
    piece = slots // wide
    block = min(256, groups // 2)
    blocks = groups // 2 // block
    flat = cap % LANES == 0
    keep = flat and 2 * groups * (a_rows + owners * cap) <= MARKS_LIMIT

    def lined(x):
        return x.reshape(-1, LANES)

    def tail(lanes):
        return max(2 * META, META * -(-cap // lanes))

    dma = pltpu.SemaphoreType.DMA
    scratch = dict(
        a_pay=pltpu.VMEM(a_payload.shape, BF16),
        b_pay=pltpu.VMEM(b_payload.shape, BF16),
        da_pay=pltpu.VMEM(da_payload.shape, BF16),
        db_pay=pltpu.VMEM(db_payload.shape, BF16),
        b_out0=pltpu.VMEM((owners, cap + tail(half), half), BF16),
        b_out1=pltpu.VMEM((owners, cap, half), BF16),
        b_in0=pltpu.VMEM((owners, cap + tail(half), half), BF16),
        b_in1=pltpu.VMEM((owners, cap, half), BF16),
        d_out=pltpu.VMEM((owners, cap + tail(width), width), BF16),
        d_in=pltpu.VMEM((owners, cap + tail(width), width), BF16),
        b_marks=pltpu.VMEM((slots, owners * cap) if flat else (owners, slots, cap), BF16),
        a_marks=pltpu.VMEM((a_rows, slots), BF16),
        d_marks=pltpu.VMEM((owners * cap, slots), BF16),
        base=pltpu.VMEM((slots, width), F32),
        base_first=pltpu.VMEM((slots, width), F32),
        base_in=pltpu.VMEM((wide, piece, width), F32),
        base_total=pltpu.VMEM((slots, width), F32),
        part=pltpu.VMEM((2, slots, half), F32),
        part_in=pltpu.VMEM((2, wide, piece, half), F32),
        part_mid=pltpu.VMEM((2, piece, half), F32),
        part_first=pltpu.VMEM((2, piece, half), F32),
        part_total=pltpu.VMEM((2, slots, half), F32),
        a_table=pltpu.VMEM((slots, width), BF16),
        d_table=pltpu.VMEM((2, slots, width), BF16),
        a_terms=pltpu.VMEM((a_rows, width), BF16),
        d_terms=pltpu.VMEM((owners * cap, width), BF16),
        a_place=pltpu.VMEM((a_rows // LANES, LANES), jnp.int32),
        view=pltpu.VMEM((groups, width), F32),
        give=pltpu.VMEM((groups // 2, width), F32),
        take=pltpu.VMEM((groups // 2, width), F32),
        pieces=pltpu.VMEM((owners * views // 2, held, width), BF16),
        inbox=pltpu.VMEM((owners * views // 2, held, width), BF16),
        load=dma((4,)),
        b_send=dma((2, owners)),
        b_recv=dma((2, owners)),
        d_send=dma((owners,)),
        d_recv=dma((owners,)),
        pair_send=dma,
        pair_recv=dma,
        base_send=dma((wide,)),
        base_recv=dma((wide,)),
        all_send=dma((wide,)),
        all_recv=dma((wide,)),
        w_send=dma((2, wide, 2)),
        w_recv=dma((2, wide, 2)),
        x_send=dma((2, 2)),
        x_recv=dma((2, 2)),
        g_send=dma((2, views, 2)),
        g_recv=dma((2, wide, 2)),
        c_send=dma((2, 2)),
        t_send=dma((2, wide, 2)),
        t_recv=dma((2, wide, 2)),
        p_send=dma((blocks,)),
        p_recv=dma((blocks,)),
        o_send=dma((owners * views // 2,)),
        o_recv=dma((owners * views // 2,)),
    )
    if keep:
        scratch["a_groups"] = pltpu.VMEM((groups, a_rows), BF16)
        scratch["d_groups"] = pltpu.VMEM((groups, owners * cap), BF16)
    dims = types.SimpleNamespace(
        names=tuple(scratch), owners=owners, views=views, cap=cap, slots=slots, groups=groups, width=width,
        held=held, keep=keep, flat=flat,
    )
    vmem, smem = pl.BlockSpec(memory_space=pltpu.VMEM), pl.BlockSpec(memory_space=pltpu.SMEM)
    away = pl.BlockSpec(memory_space=pl.ANY)
    sums = pl.pallas_call(
        functools.partial(kernel, dims),
        out_shape=pltpu.VMEM((2, held, width), F32),
        in_specs=[smem] * 2 + [vmem] * 11 + [away] * 4,
        out_specs=vmem,
        scratch_shapes=list(scratch.values()),
        compiler_params=pltpu.CompilerParams(
            collective_id=0, has_side_effects=True, vmem_limit_bytes=VMEM_LIMIT
        ),
        name="delta_view",
    )(
        da_count, db_count, lined(key_slot), lined(a_slot), lined(a_weight), lined(a_group), lined(b_slot),
        lined(b_weight), lined(da_key), lined(da_group), lined(da_mult), lined(db_key), lined(db_mult),
        a_payload, b_payload, da_payload, db_payload,
    )
    return sums[0] + sums[1]


GROUPS_DEV = 32


def solution(mesh):
    row, wide = P(("keys", "view")), P(("keys", "view"), None)
    groups = GROUPS_DEV * mesh.shape["keys"] * mesh.shape["view"]
    in_specs = (P(), row, row, row, wide, row, row, wide, row, row, row, wide, row, row, row, wide, row)
    return jax.shard_map(
        functools.partial(shards, groups), mesh=mesh, in_specs=in_specs, out_specs=wide, check_vma=False
    )
```

```python
import functools
import types

import jax
import jax.numpy as jnp
from jax import lax
from jax.experimental import pallas as pl
from jax.experimental.pallas import tpu as pltpu
from jax.sharding import PartitionSpec as P

LANES = 128
META = 8
F32 = jnp.float32
BF16 = jnp.bfloat16
VMEM_LIMIT = 62 * 1024 * 1024
MARKS_LIMIT = 16 * 1024 * 1024


def row_of(ref, start, count):
    return jnp.concatenate([ref[pl.ds(start + i, 1), :] for i in range(count)], axis=1)


def as_row(ref):
    return row_of(ref, 0, ref.shape[0])


def iota(shape, axis):
    return lax.broadcasted_iota(jnp.int32, shape, axis)


def dot(a, b):
    return jnp.dot(a, b, preferred_element_type=F32)


def hot(mask):
    return jnp.where(mask, 1.0, 0.0).astype(BF16)


def remote(src, dst, send, recv, keys, view):
    return pltpu.make_async_remote_copy(
        src_ref=src, dst_ref=dst, send_sem=send, recv_sem=recv,
        device_id=(keys, view), device_id_type=pl.DeviceIdType.MESH,
    )


def aligned(start, count):
    return pl.ds(pl.multiple_of(start, count), count)


def pack_plan(owners, keys_dev, cap, table_ref, key_ref, mult_ref, group_ref, count):
    key = as_row(key_ref)
    rows = key.shape[1]
    table = table_ref[...]
    tiles = table.shape[0]
    halves = jnp.concatenate([table & 255, table >> 8], axis=0).astype(F32).astype(BF16)
    looked = dot(halves, hot(iota((LANES, rows), 0) == (key & (LANES - 1))))
    high = iota((tiles, rows), 0) == (key >> 7)
    slot_low = jnp.sum(jnp.where(high, looked[:tiles], 0.0), axis=0, keepdims=True)
    slot_high = jnp.sum(jnp.where(high, looked[tiles:], 0.0), axis=0, keepdims=True)
    slot = slot_low.astype(jnp.int32) + 256 * slot_high.astype(jnp.int32)
    owner = slot // keys_dev
    local = slot - owner * keys_dev
    alive = iota((1, rows), 1) < count
    marks = jnp.where((iota((owners, rows), 0) == owner) & alive, 1.0, 0.0)
    step = min(256, rows)
    upper = hot(iota((step, step), 0) < iota((step, step), 1))
    running = jnp.zeros((owners, 1), F32)
    ranks = []
    for at in range(0, rows, step):
        piece = marks[:, at:at + step]
        before = dot(piece.astype(BF16), upper) + running
        ranks.append(jnp.sum(piece * before, axis=0, keepdims=True))
        running = running + jnp.sum(piece, axis=1, keepdims=True)
    rank = jnp.concatenate(ranks, axis=1).astype(jnp.int32)
    dest = jnp.where(alive, owner * cap + rank, -1)
    sign = as_row(mult_ref).astype(F32)
    parts = [local & 255, local >> 8]
    if group_ref is not None:
        group = as_row(group_ref)
        parts += [group & 255, group >> 8]
    meta = jnp.concatenate(
        [p.astype(F32) * sign for p in parts] + [jnp.zeros((META - len(parts), rows), F32)], axis=0
    ).astype(BF16)
    return dest, sign, meta


def packed(plan, cap, pay_ref, owner):
    dest, sign, meta = plan
    place = jnp.where(iota((cap, dest.shape[1]), 0) == dest - owner * cap, sign, 0.0).astype(BF16)
    columns = lax.dot_general(meta, place, (((1,), (1,)), ((), ())), preferred_element_type=F32)
    return dot(place, pay_ref[...]).astype(BF16), columns.astype(BF16)


def put_meta(ref, at, cap, columns):
    lanes = ref.shape[2]
    for t, lane in enumerate(range(0, cap, lanes)):
        wide = min(lanes, cap - lane)
        ref[at, cap + t * META:cap + (t + 1) * META, :wide] = columns[:, lane:lane + wide]


def meta_row(ref, at, row, cap):
    lanes = ref.shape[2]
    found = []
    for r in (row, row + 1):
        pieces = []
        for t, lane in enumerate(range(0, cap, lanes)):
            place = cap + t * META + r
            pieces.append(ref[at, place:place + 1, :min(lanes, cap - lane)].astype(F32))
        found.append(jnp.concatenate(pieces, axis=1).astype(jnp.int32))
    return found[0] + 256 * found[1]


def split(x):
    top = x.astype(BF16)
    return jnp.concatenate([top, (x - top.astype(F32)).astype(BF16)], axis=1)


def columns_of(row, width):
    return jnp.transpose(jnp.broadcast_to(row, (width, row.shape[1])))


def slot_marks(row, weight, keys_dev):
    count = row.shape[1]
    code = columns_of(row * 4 + weight, LANES)
    slot, scale = code >> 2, (code & 3).astype(F32)
    return jnp.concatenate(
        [
            jnp.where(iota((count, LANES), 1) + at == slot, scale, 0.0).astype(BF16)
            for at in range(0, keys_dev, LANES)
        ],
        axis=1,
    )


def kernel(d, *refs):
    da_count, db_count, *held_away, a_hbm, b_hbm, da_hbm, db_hbm, out = refs[:18]
    s = types.SimpleNamespace(**dict(zip(d.names, refs[18:], strict=True)))
    n, views, cap, slots, groups, width = d.owners, d.views, d.cap, d.slots, d.groups, d.width
    half, held = width // 2, d.held
    me, view = lax.axis_index("keys"), lax.axis_index("view")
    core = view & 1
    low = n // 2
    side = me // low
    place = me - side * low
    a_rows = s.a_pay.shape[0]

    groups_of = ((0, s.key_slot), (1, s.db_ints), (2, s.da_ints), (3, s.ab_ints))
    copies = []
    for i, to in groups_of:
        for r in range(to.shape[0]):
            copies.append(pltpu.make_async_copy(held_away[len(copies)], to.at[r], s.load.at[4 + i]))
    loads = [
        pltpu.make_async_copy(src, dst, s.load.at[i])
        for i, (src, dst) in enumerate(
            ((db_hbm, s.db_pay), (da_hbm, s.da_pay), (b_hbm, s.b_pay), (a_hbm, s.a_pay))
        )
    ]
    for load in copies[:3] + loads[:1] + copies[3:] + loads[1:]:
        load.start()

    def loaded(i):
        to = groups_of[i][1]
        pltpu.make_async_copy(to, to, s.load.at[4 + i]).wait()

    def sent(ref, semaphore):
        remote(ref, ref, semaphore, semaphore, me, view).wait_send()

    def landed(ref, semaphore):
        remote(ref, ref, semaphore, semaphore, me, view).wait_recv()

    barrier = pltpu.get_barrier_semaphore()
    devices = n * views
    mine = me * views + view

    def greet(i, carry):
        other = lax.rem(mine + i, devices)
        pl.semaphore_signal(
            barrier, inc=1, device_id=(other // views, lax.rem(other, views)),
            device_id_type=pl.DeviceIdType.MESH,
        )
        return carry

    lax.fori_loop(1, devices, greet, 0)

    loaded(0)
    loaded(1)
    b_plan = pack_plan(n, slots, cap, s.key_slot.at[0], s.db_ints.at[0], s.db_ints.at[1], None, db_count[0])
    loads[0].wait()

    from_me = core * low + place

    def row_copy(src, dst, send, recv, owner, source):
        there = owner // low
        return remote(
            src.at[owner], dst.at[source], send, recv,
            side * low + owner - there * low, (view - core) + there,
        )

    def b_copy(j, owner, source):
        src, dst = ((s.b_out0, s.b_in0), (s.b_out1, s.b_in1))[j]
        recv = s.b_recv.at[source] if j == 0 else s.b_later.at[source // low]
        return row_copy(src, dst, s.b_send.at[j], recv, owner, source)

    def d_copy(owner, source):
        return row_copy(s.d_out, s.d_in, s.d_send, s.d_recv.at[source], owner, source)

    def b_pack(low_ref, high_ref, at):
        rows, columns = packed(b_plan, cap, s.db_pay, at)
        low_ref[at, :cap, :] = rows[:, :half]
        high_ref[at, :cap, :] = rows[:, half:]
        put_meta(low_ref, at, cap, columns)

    def b_one(i, carry):
        b_pack(s.b_out0, s.b_out1, from_me ^ (n - i))
        return carry

    def b_start(j, i, carry):
        b_copy(j, from_me ^ (n - i), from_me).start()
        return carry

    def b_both(i, carry):
        b_one(i, carry)
        return b_start(0, i, carry)

    early = min(2, n)
    lax.fori_loop(1, early, b_one, 0)
    pl.semaphore_wait(barrier, devices - 1)
    lax.fori_loop(1, early, functools.partial(b_start, 0), 0)
    lax.fori_loop(early, n, b_both, 0)
    lax.fori_loop(1, n, functools.partial(b_start, 1), 0)
    b_pack(s.b_in0, s.b_in1, from_me)

    right = core == side
    wide = views // 2
    spot_x = view // 2
    piece = slots // wide
    own = aligned(spot_x * piece, piece)
    ahead = [(i - 1, lax.rem(spot_x + i, wide)) for i in range(1, wide)]
    behind = [(i - 1, lax.rem(spot_x + wide - i, wide)) for i in range(1, wide)]

    def wrong(run):
        pl.when(core != side)(run)

    base_pair = remote(s.base, s.base_first, s.pair_send, s.pair_recv, me, view ^ 1)

    def base_copy(i, p):
        at = aligned(p * piece, piece)
        return remote(s.base.at[at], s.base_in.at[i], s.base_send.at[i], s.base_recv.at[i], me, p * 2 + core)

    def base_add():
        @pl.when(right)
        def _():
            base_pair.wait_recv()
            s.base[...] += s.base_first[...]
            for i, p in ahead:
                base_copy(i, p).start()

    def base_end():
        @pl.when(right)
        def _():
            s.base_total[own, :] = s.base[own, :]
            for i, p in behind:
                base_copy(i, p).wait_recv()
                s.base_total[own, :] += s.base_in[i]

    def base_all(i, p, source):
        at = s.base_total.at[aligned(source * piece, piece)]
        return remote(at, at, s.all_send.at[i], s.all_recv.at[i], me, p * 2 + core)

    def base_spread():
        @pl.when(right)
        def _():
            for i, p in ahead:
                base_all(i, p, spot_x).start()

    sub = piece // 2
    subs = [pl.ds(q * sub, sub) for q in range(2)]

    def part_of(p, q):
        return aligned(p * piece + q * sub, sub)

    def wide_copy(j, i, p, q):
        return remote(
            s.part.at[j, part_of(p, q)], s.part_in.at[j, i, subs[q]], s.w_send, s.w_recv.at[j, i, q], me, p * 2 + core
        )

    def cross_copy(j, q):
        return remote(
            s.part_mid.at[j, subs[q]], s.part_first.at[j, subs[q]], s.x_send, s.x_recv.at[j, q], me ^ low, view
        )

    def total_copy(j, i, q):
        at = s.part_total.at[j, part_of(spot_x, q)]
        return remote(at, at, s.g_send.at[i - 1], s.g_recv.at[j, spot_x], me, lax.rem(view + i, views))

    def total_landed(j, p):
        landed(s.part_total.at[j, aligned(p * piece, piece)], s.g_recv.at[j, p])

    def table_copy(j):
        at = s.d_table.at[j, own]
        return remote(at, at, s.c_send, s.c_recv.at[j], me ^ low, view)

    def table_peer(j, i, p, source):
        at = s.d_table.at[j, aligned(source * piece, piece)]
        return remote(at, at, s.t_send, s.t_recv.at[j, i], me, p * 2 + core)

    def wide_give(j):
        for q in range(2):
            for i, p in ahead:
                wide_copy(j, i, p, q).start()

    def wide_take(j):
        for q in range(2):
            total = s.part[j, part_of(spot_x, q)]
            for i, p in behind:
                wide_copy(j, i, p, q).wait_recv()
                total += s.part_in[j, i, subs[q]]
            s.part_mid[j, subs[q]] = total
            wrong(lambda: cross_copy(j, q).start())

    def total_give(j):
        @pl.when(right)
        def _():
            for q in range(2):
                cross_copy(j, q).wait_recv()
                s.part_total[j, part_of(spot_x, q)] = s.part_mid[j, subs[q]] + s.part_first[j, subs[q]]
                for i in range(1, views):
                    total_copy(j, i, q).start()

    def table_give(j):
        @pl.when(right)
        def _():
            s.d_table[j, own] = split(s.part_total[j, own] + s.base_total[own, j * half:(j + 1) * half])
            table_copy(j).start()

    def total_take(j):
        for _, p in behind:
            total_landed(j, p)
        wrong(lambda: total_landed(j, spot_x))

    def table_relay(j):
        @wrong
        def _():
            table_copy(j).wait_recv()
            for i, p in ahead:
                table_peer(j, i, p, spot_x).start()

    def table_take(j):
        @wrong
        def _():
            for i, p in behind:
                table_peer(j, i, p, p).wait_recv()

        @pl.when(right)
        def _():
            for _, p in behind:
                at = aligned(p * piece, piece)
                s.d_table[j, at] = split(s.part_total[j, at] + s.base_total[at, j * half:(j + 1) * half])

    loaded(3)
    loads[2].wait()
    chunk = min(1024, s.b_pay.shape[0])
    lines = chunk // LANES
    s.base[...] = jnp.zeros_like(s.base)

    def base_one(c, carry):
        slot = row_of(s.ab_ints.at[0], c * lines, lines)
        weight = row_of(s.ab_ints.at[1], c * lines, lines).astype(F32)
        marks = jnp.where(iota((slots, chunk), 0) == slot, weight, 0.0).astype(BF16)
        s.base[...] += dot(marks, s.b_pay[aligned(c * chunk, chunk), :])
        return carry

    lax.fori_loop(0, s.b_pay.shape[0] // chunk, base_one, 0)
    wrong(base_pair.start)

    few = min(512, a_rows)
    few_lines = few // LANES

    def slot_one(c, carry):
        s.a_marks[aligned(c * few, few), :] = slot_marks(
            row_of(s.ab_ints.at[2], c * few_lines, few_lines), row_of(s.ab_ints.at[3], c * few_lines, few_lines), slots
        )
        return carry

    loaded(2)
    d_plan = pack_plan(
        n, slots, cap, s.key_slot.at[0], s.da_ints.at[0], s.da_ints.at[2], s.da_ints.at[1], da_count[0]
    )
    loads[1].wait()
    def d_pack(ref, at, owner):
        rows, columns = packed(d_plan, cap, s.da_pay, owner)
        ref[at, :cap, :] = rows
        put_meta(ref, at, cap, columns)

    step_z = max(1, low // 2)

    def d_fill(i, carry):
        owner = from_me ^ i
        d_pack(s.d_out, owner, owner)
        return carry

    def d_start(i, carry):
        near = lax.rem(i, step_z)
        owner = from_me ^ ((i - near) * 2 + step_z + near)
        d_copy(owner, from_me).start()
        return carry

    def d_near(i, carry):
        near = lax.rem(i, step_z)
        owner = from_me ^ ((i - near) * 2 + near)
        d_copy(owner, from_me).start()
        return carry

    lax.fori_loop(1, n, d_fill, 0)
    lax.fori_loop(1, n // 2, d_near, 0)
    d_pack(s.d_in, from_me, from_me)

    @pl.when(core == side)
    def _():
        lax.fori_loop(0, n // 2, d_start, 0)

    block = min(256, groups // 2)
    blocks = groups // 2 // block
    span = min(2048, a_rows)
    span_lines = span // LANES

    def group_place(group):
        to = group // held
        turned = (to >> 1) ^ ((1 - side) * (devices // 4))
        return turned * held + group - to * held + jnp.where((to & 1) == core, groups // 2, 0)

    s.a_place[...] = group_place(s.ab_ints[4])

    def group_marks(g, count, at):
        return hot(iota((count, at.shape[1]), 0) + g * count == at)

    def a_group_marks(g, c):
        return group_marks(g, block, row_of(s.a_place, c * span_lines, span_lines))

    def a_groups():
        if not d.keep:
            return

        def one(g, carry):
            for c in range(a_rows // span):
                s.a_groups[aligned(g * block, block), c * span:(c + 1) * span] = a_group_marks(g, c)
            return carry

        lax.fori_loop(0, 2 * blocks, one, 0)

    def delta_sum(j):
        arrived_at = (s.b_in0, s.b_in1)[j]

        def fill(source):
            marks = hot(iota((slots, cap), 0) == meta_row(s.b_in0, source, 0, cap))
            if d.flat:
                s.b_marks[:, aligned(source * cap, cap)] = marks
            else:
                s.b_marks[source] = marks

        def step(i, carry):
            source = from_me ^ (n - i)
            b_copy(0, source, source).wait_recv()
            fill(source)
            return carry

        def gather(of):
            first = of * low
            rows = arrived_at[pl.ds(first, low), :cap, :].reshape(low * cap, half)
            if d.flat:
                return dot(s.b_marks[:, aligned(first * cap, low * cap)], rows)
            return lax.fori_loop(
                first, first + low, lambda i, total: total + dot(s.b_marks[i], arrived_at[i, :cap, :]),
                jnp.zeros((slots, half), F32),
            )

        if j == 0:
            lax.fori_loop(1, n - low + 1, step, 0)
        else:
            landed(s.b_in1.at[pl.ds(0, low)], s.b_later.at[1 - core])
        s.part[j] = gather(1 - core)
        if j == 0:
            fill(from_me)
            lax.fori_loop(n - low + 1, n, step, 0)
        else:
            landed(s.b_in1.at[pl.ds(0, low - 1)], s.b_later.at[core])
        s.part[j] += gather(core)

    def a_gather(j):
        s.a_table[...] = split(s.part_total[j])
        lanes = slice(j * half, (j + 1) * half)

        def step(c, carry):
            rows = aligned(c * span, span)
            both = dot(s.a_marks[rows, :], s.a_table[...])
            s.a_terms[rows, lanes] = (
                s.a_pay[rows, lanes].astype(F32) * (both[:, :half] + both[:, half:])
            ).astype(BF16)
            return carry

        lax.fori_loop(0, a_rows // span, step, 0)

    def d_arrive(first, last, far):
        def one(source):
            rows = aligned(source * cap, cap)
            s.d_marks[rows, :] = slot_marks(meta_row(s.d_in, source, 0, cap), jnp.ones((1, cap), jnp.int32), slots)
            if d.keep:
                s.d_groups[:, rows] = group_marks(0, groups, group_place(meta_row(s.d_in, source, 2, cap)))

        if first == 0 and not far:
            one(from_me)

        def step(i, carry):
            if far:
                i = lax.rem(i + jnp.where(core == side, 0, n // 4), n // 2)
            near = lax.rem(i, step_z)
            source = from_me ^ ((i - near) * 2 + near + (step_z if far else 0))
            d_copy(source, source).wait_recv()
            one(source)
            return carry

        lax.fori_loop(first if far else max(first, 1), last, step, 0)

    def a_sum(first, last):
        def step(g, carry):
            rows = aligned(g * block, block)
            if d.keep:
                s.view[rows, :] = dot(s.a_groups[rows, :], s.a_terms[...])
            else:
                s.view[rows, :] = sum(
                    dot(a_group_marks(g, c), s.a_terms[c * span:(c + 1) * span, :]) for c in range(a_rows // span)
                )
            return carry

        lax.fori_loop(first, last, step, 0)

    base_add()
    delta_sum(0)
    wide_give(0)
    lax.fori_loop(0, a_rows // few, slot_one, 0)

    delta_sum(1)
    wide_give(1)
    wide_take(0)
    a_groups()
    base_end()
    loads[3].wait()
    wide_take(1)
    @wrong
    def _():
        lax.fori_loop(0, n // 4, d_start, 0)

    total_give(0)
    total_give(1)
    table_give(0)
    table_give(1)
    base_spread()
    d_arrive(0, n // 2, False)
    total_take(0)
    a_gather(0)
    @wrong
    def _():
        lax.fori_loop(n // 4, n // 2, d_start, 0)

    total_take(1)
    a_gather(1)
    a_sum(0, blocks)
    table_relay(0)
    a_sum(blocks, 2 * blocks)
    table_relay(1)
    d_arrive(0, n // 2, True)

    @pl.when(right)
    def _():
        for i, p in behind:
            base_all(i, p, p).wait_recv()

    for j in range(2):
        table_take(j)

    several = min(n, span // cap)

    def d_gather(c, carry):
        rows = aligned(c * several * cap, several * cap)
        for j in range(2):
            lanes = slice(j * half, (j + 1) * half)
            both = dot(s.d_marks[rows, :], s.d_table[j])
            pay = s.d_in[pl.ds(c * several, several), :cap, lanes].reshape(several * cap, half)
            s.d_terms[rows, lanes] = (pay.astype(F32) * (both[:, :half] + both[:, half:])).astype(BF16)
        return carry

    lax.fori_loop(0, n // several, d_gather, 0)

    def d_sum(g):
        rows = aligned(g * block, block)
        if d.keep:
            return s.view[rows, :] + dot(s.d_groups[rows, :], s.d_terms[...])

        def one(source, total):
            marks = group_marks(g, block, group_place(meta_row(s.d_in, source, 2, cap)))
            return total + dot(marks, s.d_terms[aligned(source * cap, cap), :])

        return lax.fori_loop(0, n, one, s.view[rows, :])

    def pair_copy(g):
        rows = aligned(g * block, block)
        return remote(s.give.at[rows], s.take.at[rows], s.p_send, s.p_recv.at[g], me, view ^ 1)

    def give_one(g, carry):
        s.give[aligned(g * block, block), :] = d_sum(g)
        pair_copy(g).start()
        return carry

    lax.fori_loop(0, blocks, give_one, 0)
    pairs = views // 2
    spot = me * pairs + view // 2
    per = block // held

    def piece_copy(to, source):
        owner = to // pairs
        return remote(
            s.pieces.at[to], s.inbox.at[source], s.o_send, s.o_recv,
            owner, (to - owner * pairs) * 2 + core,
        )

    def keep_one(g, carry):
        total = d_sum(g + blocks)
        pair_copy(g).wait_recv()
        total = (total + s.take[aligned(g * block, block), :]).astype(BF16)
        for i in range(per):
            s.pieces[(g * per + i) ^ ((1 - side) * (devices // 4))] = total[i * held:(i + 1) * held, :]

        def send(i, inner):
            to = (g * per + i) ^ ((1 - side) * (devices // 4))

            @pl.when(to != spot)
            def _():
                piece_copy(to, spot).start()
            return inner

        lax.fori_loop(0, per, send, 0)
        return carry

    lax.fori_loop(0, blocks, keep_one, 0)
    everyone = n * pairs
    others = pl.ds(0, everyone - 1)
    s.inbox[spot] = s.pieces[spot]
    landed(s.inbox.at[others], s.o_recv)
    middle = everyone // 2
    out[0] = jnp.sum(s.inbox[:middle].astype(F32), axis=0)
    out[1] = jnp.sum(s.inbox[middle:].astype(F32), axis=0)

    rest = pl.ds(0, n - 1)
    sent(s.b_out0.at[rest], s.b_send.at[0])
    sent(s.b_out1.at[rest], s.b_send.at[1])
    sent(s.d_out.at[rest], s.d_send)
    sent(s.give, s.p_send)
    sent(s.pieces.at[others], s.o_send)
    sent(s.part.at[:, pl.ds(0, (wide - 1) * piece)], s.w_send)

    @wrong
    def _():
        base_pair.wait_send()
        sent(s.part_mid, s.x_send)
        sent(s.d_table.at[:, pl.ds(0, (wide - 1) * piece)], s.t_send)

    @pl.when(right)
    def _():
        for i, p in ahead:
            base_copy(i, p).wait_send()
            base_all(i, p, spot_x).wait_send()
        for i in range(views - 1):
            sent(s.part_mid, s.g_send.at[i])
        sent(s.d_table.at[:, own], s.c_send)


def shards(
    groups, key_slot, a_slot, a_group, a_weight, a_payload, b_slot, b_weight, b_payload,
    da_key, da_group, da_mult, da_payload, da_count, db_key, db_mult, db_payload, db_count,
):
    owners, views = lax.axis_size("keys"), lax.axis_size("view")
    a_rows, width = a_payload.shape
    slots = key_slot.shape[0] // owners
    delta = da_payload.shape[0]
    cap = 2 * delta // owners
    half = width // 2
    held = groups // (owners * views)
    wide = views // 2
    piece = slots // wide
    block = min(256, groups // 2)
    blocks = groups // 2 // block
    flat = cap % LANES == 0
    keep = flat and 2 * groups * (a_rows + owners * cap) <= MARKS_LIMIT

    def lined(x):
        return x.reshape(-1, LANES)

    def tail(lanes):
        return max(2 * META, META * -(-cap // lanes))

    dma = pltpu.SemaphoreType.DMA
    ints = [
        lined(x)
        for x in (key_slot, db_key, db_mult, da_key, da_group, da_mult, b_slot, b_weight, a_slot, a_weight, a_group)
    ]
    scratch = dict(
        key_slot=pltpu.VMEM((1, *ints[0].shape), jnp.int32),
        db_ints=pltpu.VMEM((2, *ints[1].shape), jnp.int32),
        da_ints=pltpu.VMEM((3, *ints[3].shape), jnp.int32),
        ab_ints=pltpu.VMEM((5, *ints[6].shape), jnp.int32),
        a_pay=pltpu.VMEM(a_payload.shape, BF16),
        b_pay=pltpu.VMEM(b_payload.shape, BF16),
        da_pay=pltpu.VMEM(da_payload.shape, BF16),
        db_pay=pltpu.VMEM(db_payload.shape, BF16),
        b_out0=pltpu.VMEM((owners, cap + tail(half), half), BF16),
        b_out1=pltpu.VMEM((owners, cap, half), BF16),
        b_in0=pltpu.VMEM((owners, cap + tail(half), half), BF16),
        b_in1=pltpu.VMEM((owners, cap, half), BF16),
        d_out=pltpu.VMEM((owners, cap + tail(width), width), BF16),
        d_in=pltpu.VMEM((owners, cap + tail(width), width), BF16),
        b_marks=pltpu.VMEM((slots, owners * cap) if flat else (owners, slots, cap), BF16),
        a_marks=pltpu.VMEM((a_rows, slots), BF16),
        d_marks=pltpu.VMEM((owners * cap, slots), BF16),
        base=pltpu.VMEM((slots, width), F32),
        base_first=pltpu.VMEM((slots, width), F32),
        base_in=pltpu.VMEM((wide - 1, piece, width), F32),
        base_total=pltpu.VMEM((slots, width), F32),
        part=pltpu.VMEM((2, slots, half), F32),
        part_in=pltpu.VMEM((2, wide - 1, piece, half), F32),
        part_mid=pltpu.VMEM((2, piece, half), F32),
        part_first=pltpu.VMEM((2, piece, half), F32),
        part_total=pltpu.VMEM((2, slots, half), F32),
        a_table=pltpu.VMEM((slots, width), BF16),
        d_table=pltpu.VMEM((2, slots, width), BF16),
        a_terms=pltpu.VMEM((a_rows, width), BF16),
        d_terms=pltpu.VMEM((owners * cap, width), BF16),
        a_place=pltpu.VMEM((a_rows // LANES, LANES), jnp.int32),
        view=pltpu.VMEM((groups, width), F32),
        give=pltpu.VMEM((groups // 2, width), F32),
        take=pltpu.VMEM((groups // 2, width), F32),
        pieces=pltpu.VMEM((owners * views // 2, held, width), BF16),
        inbox=pltpu.VMEM((owners * views // 2, held, width), BF16),
        load=dma((8,)),
        b_send=dma((2,)),
        b_recv=dma((owners,)),
        b_later=dma((2,)),
        d_send=dma,
        d_recv=dma((owners,)),
        pair_send=dma,
        pair_recv=dma,
        base_send=dma((wide - 1,)),
        base_recv=dma((wide - 1,)),
        all_send=dma((wide - 1,)),
        all_recv=dma((wide - 1,)),
        w_send=dma,
        w_recv=dma((2, wide - 1, 2)),
        x_send=dma,
        x_recv=dma((2, 2)),
        g_send=dma((views - 1,)),
        g_recv=dma((2, wide)),
        c_send=dma,
        c_recv=dma((2,)),
        t_send=dma,
        t_recv=dma((2, wide - 1)),
        p_send=dma,
        p_recv=dma((blocks,)),
        o_send=dma,
        o_recv=dma,
    )
    if keep:
        scratch["a_groups"] = pltpu.VMEM((groups, a_rows), BF16)
        scratch["d_groups"] = pltpu.VMEM((groups, owners * cap), BF16)
    dims = types.SimpleNamespace(
        names=tuple(scratch), owners=owners, views=views, cap=cap, slots=slots, groups=groups, width=width,
        held=held, keep=keep, flat=flat,
    )
    vmem, smem = pl.BlockSpec(memory_space=pltpu.VMEM), pl.BlockSpec(memory_space=pltpu.SMEM)
    away = pl.BlockSpec(memory_space=pl.ANY)
    sums = pl.pallas_call(
        functools.partial(kernel, dims),
        out_shape=pltpu.VMEM((2, held, width), F32),
        in_specs=[smem] * 2 + [away] * 15,
        out_specs=vmem,
        scratch_shapes=list(scratch.values()),
        compiler_params=pltpu.CompilerParams(
            collective_id=0, has_side_effects=True, vmem_limit_bytes=VMEM_LIMIT
        ),
        name="delta_view",
    )(
        da_count, db_count, *ints,
        a_payload, b_payload, da_payload, db_payload,
    )
    return sums[0] + sums[1]


GROUPS_DEV = 32


def solution(mesh):
    row, wide = P(("keys", "view")), P(("keys", "view"), None)
    groups = GROUPS_DEV * mesh.shape["keys"] * mesh.shape["view"]
    in_specs = (P(), row, row, row, wide, row, row, wide, row, row, row, wide, row, row, row, wide, row)
    return jax.shard_map(
        functools.partial(shards, groups), mesh=mesh, in_specs=in_specs, out_specs=wide, check_vma=False
    )
```

```python
import functools
import types

import jax
import jax.numpy as jnp
from jax import lax
from jax.experimental import pallas as pl
from jax.experimental.pallas import tpu as pltpu
from jax.sharding import PartitionSpec as P

LANES = 128
META = 8
F32 = jnp.float32
BF16 = jnp.bfloat16
VMEM_LIMIT = 62 * 1024 * 1024
MARKS_LIMIT = 16 * 1024 * 1024


def row_of(ref, start, count):
    return jnp.concatenate([ref[pl.ds(start + i, 1), :] for i in range(count)], axis=1)


def as_row(ref):
    return row_of(ref, 0, ref.shape[0])


def iota(shape, axis):
    return lax.broadcasted_iota(jnp.int32, shape, axis)


def dot(a, b):
    return jnp.dot(a, b, preferred_element_type=F32)


def hot(mask):
    return jnp.where(mask, 1.0, 0.0).astype(BF16)


def remote(src, dst, send, recv, keys, view):
    return pltpu.make_async_remote_copy(
        src_ref=src, dst_ref=dst, send_sem=send, recv_sem=recv,
        device_id=(keys, view), device_id_type=pl.DeviceIdType.MESH,
    )


def aligned(start, count):
    return pl.ds(pl.multiple_of(start, count), count)


def pack_plan(owners, keys_dev, cap, table_ref, key_ref, mult_ref, group_ref, count):
    key = as_row(key_ref)
    rows = key.shape[1]
    table = table_ref[...]
    tiles = table.shape[0]
    halves = jnp.concatenate([table & 255, table >> 8], axis=0).astype(F32).astype(BF16)
    looked = dot(halves, hot(iota((LANES, rows), 0) == (key & (LANES - 1))))
    high = iota((tiles, rows), 0) == (key >> 7)
    slot_low = jnp.sum(jnp.where(high, looked[:tiles], 0.0), axis=0, keepdims=True)
    slot_high = jnp.sum(jnp.where(high, looked[tiles:], 0.0), axis=0, keepdims=True)
    slot = slot_low.astype(jnp.int32) + 256 * slot_high.astype(jnp.int32)
    owner = slot // keys_dev
    local = slot - owner * keys_dev
    alive = iota((1, rows), 1) < count
    marks = jnp.where((iota((owners, rows), 0) == owner) & alive, 1.0, 0.0)
    step = min(256, rows)
    upper = hot(iota((step, step), 0) < iota((step, step), 1))
    running = jnp.zeros((owners, 1), F32)
    ranks = []
    for at in range(0, rows, step):
        piece = marks[:, at:at + step]
        before = dot(piece.astype(BF16), upper) + running
        ranks.append(jnp.sum(piece * before, axis=0, keepdims=True))
        running = running + jnp.sum(piece, axis=1, keepdims=True)
    rank = jnp.concatenate(ranks, axis=1).astype(jnp.int32)
    dest = jnp.where(alive, owner * cap + rank, -1)
    sign = as_row(mult_ref).astype(F32)
    parts = [local & 255, local >> 8]
    if group_ref is not None:
        group = as_row(group_ref)
        parts += [group & 255, group >> 8]
    meta = jnp.concatenate(
        [p.astype(F32) * sign for p in parts] + [jnp.zeros((META - len(parts), rows), F32)], axis=0
    ).astype(BF16)
    return dest, sign, meta


def packed(plan, cap, pay_ref, owner):
    dest, sign, meta = plan
    place = jnp.where(iota((cap, dest.shape[1]), 0) == dest - owner * cap, sign, 0.0).astype(BF16)
    columns = lax.dot_general(meta, place, (((1,), (1,)), ((), ())), preferred_element_type=F32)
    return dot(place, pay_ref[...]).astype(BF16), columns.astype(BF16)


def put_meta(ref, at, cap, columns):
    lanes = ref.shape[2]
    for t, lane in enumerate(range(0, cap, lanes)):
        wide = min(lanes, cap - lane)
        ref[at, cap + t * META:cap + (t + 1) * META, :wide] = columns[:, lane:lane + wide]


def meta_row(ref, at, row, cap):
    lanes = ref.shape[2]
    found = []
    for r in (row, row + 1):
        pieces = []
        for t, lane in enumerate(range(0, cap, lanes)):
            place = cap + t * META + r
            pieces.append(ref[at, place:place + 1, :min(lanes, cap - lane)].astype(F32))
        found.append(jnp.concatenate(pieces, axis=1).astype(jnp.int32))
    return found[0] + 256 * found[1]


def split(x):
    top = x.astype(BF16)
    return jnp.concatenate([top, (x - top.astype(F32)).astype(BF16)], axis=1)


def columns_of(row, width):
    return jnp.transpose(jnp.broadcast_to(row, (width, row.shape[1])))


def slot_marks(row, weight, keys_dev):
    count = row.shape[1]
    code = columns_of(row * 4 + weight, LANES)
    slot, scale = code >> 2, (code & 3).astype(F32)
    return jnp.concatenate(
        [
            jnp.where(iota((count, LANES), 1) + at == slot, scale, 0.0).astype(BF16)
            for at in range(0, keys_dev, LANES)
        ],
        axis=1,
    )


def kernel(d, *refs):
    da_count, db_count, *held_away, a_hbm, b_hbm, da_hbm, db_hbm, out = refs[:18]
    s = types.SimpleNamespace(**dict(zip(d.names, refs[18:], strict=True)))
    n, views, cap, slots, groups, width = d.owners, d.views, d.cap, d.slots, d.groups, d.width
    half, held = width // 2, d.held
    me, view = lax.axis_index("keys"), lax.axis_index("view")
    core = view & 1
    low = n // 2
    side = me // low
    place = me - side * low
    a_rows = s.a_pay.shape[0]

    groups_of = ((0, s.key_slot), (1, s.db_ints), (2, s.da_ints), (3, s.ab_ints))
    copies = []
    for i, to in groups_of:
        for r in range(to.shape[0]):
            copies.append(pltpu.make_async_copy(held_away[len(copies)], to.at[r], s.load.at[4 + i]))
    loads = [
        pltpu.make_async_copy(src, dst, s.load.at[i])
        for i, (src, dst) in enumerate(
            ((db_hbm, s.db_pay), (da_hbm, s.da_pay), (b_hbm, s.b_pay), (a_hbm, s.a_pay))
        )
    ]
    for load in copies[:3] + loads[:1] + copies[3:] + loads[1:]:
        load.start()

    def loaded(i):
        to = groups_of[i][1]
        pltpu.make_async_copy(to, to, s.load.at[4 + i]).wait()

    def sent(ref, semaphore):
        remote(ref, ref, semaphore, semaphore, me, view).wait_send()

    def landed(ref, semaphore):
        remote(ref, ref, semaphore, semaphore, me, view).wait_recv()

    barrier = pltpu.get_barrier_semaphore()
    devices = n * views
    mine = me * views + view

    def greet(i, carry):
        other = lax.rem(mine + i, devices)
        pl.semaphore_signal(
            barrier, inc=1, device_id=(other // views, lax.rem(other, views)),
            device_id_type=pl.DeviceIdType.MESH,
        )
        return carry

    lax.fori_loop(1, devices, greet, 0)

    loaded(0)
    loaded(1)
    b_plan = pack_plan(n, slots, cap, s.key_slot.at[0], s.db_ints.at[0], s.db_ints.at[1], None, db_count[0])
    loads[0].wait()

    from_me = core * low + place

    def row_copy(src, dst, send, recv, owner, source):
        there = owner // low
        return remote(
            src.at[owner], dst.at[source], send, recv,
            side * low + owner - there * low, (view - core) + there,
        )

    def b_copy(j, owner, source):
        src, dst = ((s.b_out0, s.b_in0), (s.b_out1, s.b_in1))[j]
        recv = s.b_recv.at[source] if j == 0 else s.b_later.at[source // low]
        return row_copy(src, dst, s.b_send.at[j], recv, owner, source)

    def d_copy(owner, source):
        return row_copy(s.d_out, s.d_in, s.d_send, s.d_recv.at[source], owner, source)

    def b_pack(low_ref, high_ref, at):
        rows, columns = packed(b_plan, cap, s.db_pay, at)
        low_ref[at, :cap, :] = rows[:, :half]
        high_ref[at, :cap, :] = rows[:, half:]
        put_meta(low_ref, at, cap, columns)

    def b_one(i, carry):
        b_pack(s.b_out0, s.b_out1, from_me ^ (n - i))
        return carry

    def b_start(j, i, carry):
        b_copy(j, from_me ^ (n - i), from_me).start()
        return carry

    def b_both(i, carry):
        b_one(i, carry)
        return b_start(0, i, carry)

    early = min(2, n)
    lax.fori_loop(1, early, b_one, 0)
    pl.semaphore_wait(barrier, devices - 1)
    lax.fori_loop(1, early, functools.partial(b_start, 0), 0)
    lax.fori_loop(early, n, b_both, 0)
    lax.fori_loop(1, n, functools.partial(b_start, 1), 0)
    b_pack(s.b_in0, s.b_in1, from_me)

    right = core == side
    wide = views // 2
    spot_x = view // 2
    piece = slots // wide
    own = aligned(spot_x * piece, piece)
    ahead = [(i - 1, lax.rem(spot_x + i, wide)) for i in range(1, wide)]
    behind = [(i - 1, lax.rem(spot_x + wide - i, wide)) for i in range(1, wide)]

    def wrong(run):
        pl.when(core != side)(run)

    base_pair = remote(s.base, s.base_first, s.pair_send, s.pair_recv, me, view ^ 1)

    def base_copy(i, p):
        at = aligned(p * piece, piece)
        return remote(s.base.at[at], s.base_in.at[i], s.base_send.at[i], s.base_recv.at[i], me, p * 2 + core)

    def base_add():
        @pl.when(right)
        def _():
            base_pair.wait_recv()
            s.base[...] += s.base_first[...]
            for i, p in ahead:
                base_copy(i, p).start()

    def base_end():
        @pl.when(right)
        def _():
            s.base_total[own, :] = s.base[own, :]
            for i, p in behind:
                base_copy(i, p).wait_recv()
                s.base_total[own, :] += s.base_in[i]

    def base_all(i, p, source):
        at = s.base_total.at[aligned(source * piece, piece)]
        return remote(at, at, s.all_send.at[i], s.all_recv.at[i], me, p * 2 + core)

    def base_spread():
        @pl.when(right)
        def _():
            for i, p in ahead:
                base_all(i, p, spot_x).start()

    sub = piece // 2
    subs = [pl.ds(q * sub, sub) for q in range(2)]

    def part_of(p, q):
        return aligned(p * piece + q * sub, sub)

    def wide_copy(j, i, p, q):
        return remote(
            s.part.at[j, part_of(p, q)], s.part_in.at[j, i, subs[q]], s.w_send, s.w_recv.at[j, i, q], me, p * 2 + core
        )

    def cross_copy(j, q):
        return remote(
            s.part_mid.at[j, subs[q]], s.part_first.at[j, subs[q]], s.x_send, s.x_recv.at[j, q], me ^ low, view
        )

    def total_copy(j, i, q):
        at = s.part_total.at[j, part_of(spot_x, q)]
        return remote(at, at, s.g_send.at[i - 1], s.g_recv.at[j, spot_x], me, lax.rem(view + i, views))

    def total_landed(j, p):
        landed(s.part_total.at[j, aligned(p * piece, piece)], s.g_recv.at[j, p])

    def table_copy(j):
        at = s.d_table.at[j, own]
        return remote(at, at, s.c_send, s.c_recv.at[j], me ^ low, view)

    def table_peer(j, i, p, source):
        at = s.d_table.at[j, aligned(source * piece, piece)]
        return remote(at, at, s.t_send, s.t_recv.at[j, i], me, p * 2 + core)

    def wide_give(j):
        for q in range(2):
            for i, p in ahead:
                wide_copy(j, i, p, q).start()

    def wide_take(j):
        for q in range(2):
            total = s.part[j, part_of(spot_x, q)]
            for i, p in behind:
                wide_copy(j, i, p, q).wait_recv()
                total += s.part_in[j, i, subs[q]]
            s.part_mid[j, subs[q]] = total
            wrong(lambda: cross_copy(j, q).start())

    def total_give(j):
        @pl.when(right)
        def _():
            for q in range(2):
                cross_copy(j, q).wait_recv()
                s.part_total[j, part_of(spot_x, q)] = s.part_mid[j, subs[q]] + s.part_first[j, subs[q]]
                for i in range(1, views):
                    total_copy(j, i, q).start()
                if j == 1:
                    table_give(q)

    def table_give(j):
        s.d_table[j, own] = split(s.part_total[j, own] + s.base_total[own, j * half:(j + 1) * half])
        table_copy(j).start()

    def total_take(j):
        for _, p in behind:
            total_landed(j, p)
        wrong(lambda: total_landed(j, spot_x))

    def table_relay(j):
        @wrong
        def _():
            table_copy(j).wait_recv()
            for i, p in ahead:
                table_peer(j, i, p, spot_x).start()

    def table_take(j):
        @wrong
        def _():
            for i, p in behind:
                table_peer(j, i, p, p).wait_recv()

        @pl.when(right)
        def _():
            for _, p in behind:
                at = aligned(p * piece, piece)
                s.d_table[j, at] = split(s.part_total[j, at] + s.base_total[at, j * half:(j + 1) * half])

    loaded(3)
    loads[2].wait()
    chunk = min(1024, s.b_pay.shape[0])
    lines = chunk // LANES
    s.base[...] = jnp.zeros_like(s.base)

    def base_one(c, carry):
        slot = row_of(s.ab_ints.at[0], c * lines, lines)
        weight = row_of(s.ab_ints.at[1], c * lines, lines).astype(F32)
        marks = jnp.where(iota((slots, chunk), 0) == slot, weight, 0.0).astype(BF16)
        s.base[...] += dot(marks, s.b_pay[aligned(c * chunk, chunk), :])
        return carry

    lax.fori_loop(0, s.b_pay.shape[0] // chunk, base_one, 0)
    wrong(base_pair.start)

    few = min(512, a_rows)
    few_lines = few // LANES

    def slot_one(c, carry):
        s.a_marks[aligned(c * few, few), :] = slot_marks(
            row_of(s.ab_ints.at[2], c * few_lines, few_lines), row_of(s.ab_ints.at[3], c * few_lines, few_lines), slots
        )
        return carry

    loaded(2)
    d_plan = pack_plan(
        n, slots, cap, s.key_slot.at[0], s.da_ints.at[0], s.da_ints.at[2], s.da_ints.at[1], da_count[0]
    )
    loads[1].wait()
    def d_pack(ref, at, owner):
        rows, columns = packed(d_plan, cap, s.da_pay, owner)
        ref[at, :cap, :] = rows
        put_meta(ref, at, cap, columns)

    step_z = max(1, low // 2)

    def d_fill(i, carry):
        owner = from_me ^ i
        d_pack(s.d_out, owner, owner)
        return carry

    def d_start(i, carry):
        near = lax.rem(i, step_z)
        owner = from_me ^ ((i - near) * 2 + step_z + near)
        d_copy(owner, from_me).start()
        return carry

    def d_near(i, carry):
        near = lax.rem(i, step_z)
        owner = from_me ^ ((i - near) * 2 + near)
        d_copy(owner, from_me).start()
        return carry

    lax.fori_loop(1, n, d_fill, 0)
    lax.fori_loop(1, n // 2, d_near, 0)
    d_pack(s.d_in, from_me, from_me)

    @pl.when(core == side)
    def _():
        lax.fori_loop(0, n // 2, d_start, 0)

    block = min(256, groups // 2)
    blocks = groups // 2 // block
    span = min(2048, a_rows)
    span_lines = span // LANES

    def group_place(group):
        to = group // held
        turned = (to >> 1) ^ ((1 - side) * (devices // 4))
        return turned * held + group - to * held + jnp.where((to & 1) == core, groups // 2, 0)

    s.a_place[...] = group_place(s.ab_ints[4])

    def group_marks(g, count, at):
        return hot(iota((count, at.shape[1]), 0) + g * count == at)

    def a_group_marks(g, c):
        return group_marks(g, block, row_of(s.a_place, c * span_lines, span_lines))

    def a_groups():
        if not d.keep:
            return

        def one(g, carry):
            for c in range(a_rows // span):
                s.a_groups[aligned(g * block, block), c * span:(c + 1) * span] = a_group_marks(g, c)
            return carry

        lax.fori_loop(0, 2 * blocks, one, 0)

    def delta_sum(j):
        arrived_at = (s.b_in0, s.b_in1)[j]

        def fill(source):
            marks = hot(iota((slots, cap), 0) == meta_row(s.b_in0, source, 0, cap))
            if d.flat:
                s.b_marks[:, aligned(source * cap, cap)] = marks
            else:
                s.b_marks[source] = marks

        def step(i, carry):
            source = from_me ^ (n - i)
            b_copy(0, source, source).wait_recv()
            fill(source)
            return carry

        def gather(of):
            first = of * low
            rows = arrived_at[pl.ds(first, low), :cap, :].reshape(low * cap, half)
            if d.flat:
                return dot(s.b_marks[:, aligned(first * cap, low * cap)], rows)
            return lax.fori_loop(
                first, first + low, lambda i, total: total + dot(s.b_marks[i], arrived_at[i, :cap, :]),
                jnp.zeros((slots, half), F32),
            )

        if j == 0:
            lax.fori_loop(1, n - low + 1, step, 0)
        else:
            landed(s.b_in1.at[pl.ds(0, low)], s.b_later.at[1 - core])
        s.part[j] = gather(1 - core)
        if j == 0:
            fill(from_me)
            lax.fori_loop(n - low + 1, n, step, 0)
        else:
            landed(s.b_in1.at[pl.ds(0, low - 1)], s.b_later.at[core])
        s.part[j] += gather(core)

    def a_gather(j):
        s.a_table[...] = split(s.part_total[j])
        lanes = slice(j * half, (j + 1) * half)

        def step(c, carry):
            rows = aligned(c * span, span)
            both = dot(s.a_marks[rows, :], s.a_table[...])
            s.a_terms[rows, lanes] = (
                s.a_pay[rows, lanes].astype(F32) * (both[:, :half] + both[:, half:])
            ).astype(BF16)
            return carry

        lax.fori_loop(0, a_rows // span, step, 0, unroll=True)

    def d_arrive(first, last, far):
        def one(source):
            rows = aligned(source * cap, cap)
            s.d_marks[rows, :] = slot_marks(meta_row(s.d_in, source, 0, cap), jnp.ones((1, cap), jnp.int32), slots)
            if d.keep:
                s.d_groups[:, rows] = group_marks(0, groups, group_place(meta_row(s.d_in, source, 2, cap)))

        if first == 0 and not far:
            one(from_me)

        def step(i, carry):
            if far:
                i = lax.rem(i + jnp.where(core == side, 0, n // 4), n // 2)
            near = lax.rem(i, step_z)
            source = from_me ^ ((i - near) * 2 + near + (step_z if far else 0))
            d_copy(source, source).wait_recv()
            one(source)
            return carry

        lax.fori_loop(first if far else max(first, 1), last, step, 0)

    def a_sum(first, last):
        def step(g, carry):
            rows = aligned(g * block, block)
            if d.keep:
                s.view[rows, :] = dot(s.a_groups[rows, :], s.a_terms[...])
            else:
                s.view[rows, :] = sum(
                    dot(a_group_marks(g, c), s.a_terms[c * span:(c + 1) * span, :]) for c in range(a_rows // span)
                )
            return carry

        lax.fori_loop(first, last, step, 0, unroll=True)

    delta_sum(0)
    wide_give(0)
    lax.fori_loop(0, a_rows // few, slot_one, 0)

    delta_sum(1)
    wide_give(1)
    base_add()
    wide_take(0)
    a_groups()
    wide_take(1)
    @wrong
    def _():
        lax.fori_loop(0, n // 4, d_start, 0)

    total_give(0)
    base_end()
    loads[3].wait()
    total_give(1)
    base_spread()
    d_arrive(0, n // 2, False)
    total_take(0)
    a_gather(0)
    @wrong
    def _():
        lax.fori_loop(n // 4, n // 2, d_start, 0)

    d_arrive(0, n // 4, True)
    total_take(1)
    a_gather(1)
    table_relay(0)
    a_sum(0, blocks)
    table_relay(1)
    a_sum(blocks, 2 * blocks)
    d_arrive(n // 4, n // 2, True)

    @pl.when(right)
    def _():
        for i, p in behind:
            base_all(i, p, p).wait_recv()

    several = min(n, span // cap)

    def d_gather(c, carry):
        rows = aligned(c * several * cap, several * cap)
        for j in range(2):
            lanes = slice(j * half, (j + 1) * half)
            both = dot(s.d_marks[rows, :], s.d_table[j])
            pay = s.d_in[pl.ds(c * several, several), :cap, lanes].reshape(several * cap, half)
            s.d_terms[rows, lanes] = (pay.astype(F32) * (both[:, :half] + both[:, half:])).astype(BF16)
        return carry

    table_take(0)
    table_take(1)
    lax.fori_loop(0, n // several, d_gather, 0)

    def d_sum(g):
        rows = aligned(g * block, block)
        if d.keep:
            return s.view[rows, :] + dot(s.d_groups[rows, :], s.d_terms[...])

        def one(source, total):
            marks = group_marks(g, block, group_place(meta_row(s.d_in, source, 2, cap)))
            return total + dot(marks, s.d_terms[aligned(source * cap, cap), :])

        return lax.fori_loop(0, n, one, s.view[rows, :])

    def pair_copy(g):
        rows = aligned(g * block, block)
        return remote(s.give.at[rows], s.take.at[rows], s.p_send, s.p_recv.at[g], me, view ^ 1)

    def give_one(g, carry):
        s.give[aligned(g * block, block), :] = d_sum(g)
        pair_copy(g).start()
        return carry

    lax.fori_loop(0, blocks, give_one, 0)
    pairs = views // 2
    spot = me * pairs + view // 2
    per = block // held

    def piece_copy(to, source):
        owner = to // pairs
        return remote(
            s.pieces.at[to], s.inbox.at[source], s.o_send, s.o_recv,
            owner, (to - owner * pairs) * 2 + core,
        )

    def keep_one(g, carry):
        total = d_sum(g + blocks)
        pair_copy(g).wait_recv()
        total = (total + s.take[aligned(g * block, block), :]).astype(BF16)
        for i in range(per):
            s.pieces[(g * per + i) ^ ((1 - side) * (devices // 4))] = total[i * held:(i + 1) * held, :]

        def send(i, inner):
            to = (g * per + i) ^ ((1 - side) * (devices // 4))

            @pl.when(to != spot)
            def _():
                piece_copy(to, spot).start()
            return inner

        lax.fori_loop(0, per, send, 0)
        return carry

    lax.fori_loop(0, blocks, keep_one, 0)
    everyone = n * pairs
    others = pl.ds(0, everyone - 1)
    s.inbox[spot] = s.pieces[spot]
    landed(s.inbox.at[others], s.o_recv)
    middle = everyone // 2
    out[0] = jnp.sum(s.inbox[:middle].astype(F32), axis=0)
    out[1] = jnp.sum(s.inbox[middle:].astype(F32), axis=0)

    rest = pl.ds(0, n - 1)
    sent(s.b_out0.at[rest], s.b_send.at[0])
    sent(s.b_out1.at[rest], s.b_send.at[1])
    sent(s.d_out.at[rest], s.d_send)
    sent(s.give, s.p_send)
    sent(s.pieces.at[others], s.o_send)
    sent(s.part.at[:, pl.ds(0, (wide - 1) * piece)], s.w_send)

    @wrong
    def _():
        base_pair.wait_send()
        sent(s.part_mid, s.x_send)
        sent(s.d_table.at[:, pl.ds(0, (wide - 1) * piece)], s.t_send)

    @pl.when(right)
    def _():
        for i, p in ahead:
            base_copy(i, p).wait_send()
            base_all(i, p, spot_x).wait_send()
        for i in range(views - 1):
            sent(s.part_mid, s.g_send.at[i])
        sent(s.d_table.at[:, own], s.c_send)


def shards(
    groups, key_slot, a_slot, a_group, a_weight, a_payload, b_slot, b_weight, b_payload,
    da_key, da_group, da_mult, da_payload, da_count, db_key, db_mult, db_payload, db_count,
):
    owners, views = lax.axis_size("keys"), lax.axis_size("view")
    a_rows, width = a_payload.shape
    slots = key_slot.shape[0] // owners
    delta = da_payload.shape[0]
    cap = 2 * delta // owners
    half = width // 2
    held = groups // (owners * views)
    wide = views // 2
    piece = slots // wide
    block = min(256, groups // 2)
    blocks = groups // 2 // block
    flat = cap % LANES == 0
    keep = flat and 2 * groups * (a_rows + owners * cap) <= MARKS_LIMIT

    def lined(x):
        return x.reshape(-1, LANES)

    def tail(lanes):
        return max(2 * META, META * -(-cap // lanes))

    dma = pltpu.SemaphoreType.DMA
    ints = [
        lined(x)
        for x in (key_slot, db_key, db_mult, da_key, da_group, da_mult, b_slot, b_weight, a_slot, a_weight, a_group)
    ]
    scratch = dict(
        key_slot=pltpu.VMEM((1, *ints[0].shape), jnp.int32),
        db_ints=pltpu.VMEM((2, *ints[1].shape), jnp.int32),
        da_ints=pltpu.VMEM((3, *ints[3].shape), jnp.int32),
        ab_ints=pltpu.VMEM((5, *ints[6].shape), jnp.int32),
        a_pay=pltpu.VMEM(a_payload.shape, BF16),
        b_pay=pltpu.VMEM(b_payload.shape, BF16),
        da_pay=pltpu.VMEM(da_payload.shape, BF16),
        db_pay=pltpu.VMEM(db_payload.shape, BF16),
        b_out0=pltpu.VMEM((owners, cap + tail(half), half), BF16),
        b_out1=pltpu.VMEM((owners, cap, half), BF16),
        b_in0=pltpu.VMEM((owners, cap + tail(half), half), BF16),
        b_in1=pltpu.VMEM((owners, cap, half), BF16),
        d_out=pltpu.VMEM((owners, cap + tail(width), width), BF16),
        d_in=pltpu.VMEM((owners, cap + tail(width), width), BF16),
        b_marks=pltpu.VMEM((slots, owners * cap) if flat else (owners, slots, cap), BF16),
        a_marks=pltpu.VMEM((a_rows, slots), BF16),
        d_marks=pltpu.VMEM((owners * cap, slots), BF16),
        base=pltpu.VMEM((slots, width), F32),
        base_first=pltpu.VMEM((slots, width), F32),
        base_in=pltpu.VMEM((wide - 1, piece, width), F32),
        base_total=pltpu.VMEM((slots, width), F32),
        part=pltpu.VMEM((2, slots, half), F32),
        part_in=pltpu.VMEM((2, wide - 1, piece, half), F32),
        part_mid=pltpu.VMEM((2, piece, half), F32),
        part_first=pltpu.VMEM((2, piece, half), F32),
        part_total=pltpu.VMEM((2, slots, half), F32),
        a_table=pltpu.VMEM((slots, width), BF16),
        d_table=pltpu.VMEM((2, slots, width), BF16),
        a_terms=pltpu.VMEM((a_rows, width), BF16),
        d_terms=pltpu.VMEM((owners * cap, width), BF16),
        a_place=pltpu.VMEM((a_rows // LANES, LANES), jnp.int32),
        view=pltpu.VMEM((groups, width), F32),
        give=pltpu.VMEM((groups // 2, width), F32),
        take=pltpu.VMEM((groups // 2, width), F32),
        pieces=pltpu.VMEM((owners * views // 2, held, width), BF16),
        inbox=pltpu.VMEM((owners * views // 2, held, width), BF16),
        load=dma((8,)),
        b_send=dma((2,)),
        b_recv=dma((owners,)),
        b_later=dma((2,)),
        d_send=dma,
        d_recv=dma((owners,)),
        pair_send=dma,
        pair_recv=dma,
        base_send=dma((wide - 1,)),
        base_recv=dma((wide - 1,)),
        all_send=dma((wide - 1,)),
        all_recv=dma((wide - 1,)),
        w_send=dma,
        w_recv=dma((2, wide - 1, 2)),
        x_send=dma,
        x_recv=dma((2, 2)),
        g_send=dma((views - 1,)),
        g_recv=dma((2, wide)),
        c_send=dma,
        c_recv=dma((2,)),
        t_send=dma,
        t_recv=dma((2, wide - 1)),
        p_send=dma,
        p_recv=dma((blocks,)),
        o_send=dma,
        o_recv=dma,
    )
    if keep:
        scratch["a_groups"] = pltpu.VMEM((groups, a_rows), BF16)
        scratch["d_groups"] = pltpu.VMEM((groups, owners * cap), BF16)
    dims = types.SimpleNamespace(
        names=tuple(scratch), owners=owners, views=views, cap=cap, slots=slots, groups=groups, width=width,
        held=held, keep=keep, flat=flat,
    )
    vmem, smem = pl.BlockSpec(memory_space=pltpu.VMEM), pl.BlockSpec(memory_space=pltpu.SMEM)
    away = pl.BlockSpec(memory_space=pl.ANY)
    sums = pl.pallas_call(
        functools.partial(kernel, dims),
        out_shape=pltpu.VMEM((2, held, width), F32),
        in_specs=[smem] * 2 + [away] * 15,
        out_specs=vmem,
        scratch_shapes=list(scratch.values()),
        compiler_params=pltpu.CompilerParams(
            collective_id=0, has_side_effects=True, vmem_limit_bytes=VMEM_LIMIT
        ),
        name="delta_view",
    )(
        da_count, db_count, *ints,
        a_payload, b_payload, da_payload, db_payload,
    )
    return sums[0] + sums[1]


GROUPS_DEV = 32


def solution(mesh):
    row, wide = P(("keys", "view")), P(("keys", "view"), None)
    groups = GROUPS_DEV * mesh.shape["keys"] * mesh.shape["view"]
    in_specs = (P(), row, row, row, wide, row, row, wide, row, row, row, wide, row, row, row, wide, row)
    return jax.shard_map(
        functools.partial(shards, groups), mesh=mesh, in_specs=in_specs, out_specs=wide, check_vma=False
    )
```

```python
import functools
import types

import jax
import jax.numpy as jnp
from jax import lax
from jax.experimental import pallas as pl
from jax.experimental.pallas import tpu as pltpu
from jax.sharding import PartitionSpec as P

LANES = 128
META = 8
F32 = jnp.float32
BF16 = jnp.bfloat16
VMEM_LIMIT = 62 * 1024 * 1024
MARKS_LIMIT = 16 * 1024 * 1024


def row_of(ref, start, count):
    return jnp.concatenate([ref[pl.ds(start + i, 1), :] for i in range(count)], axis=1)


def as_row(ref):
    return row_of(ref, 0, ref.shape[0])


def iota(shape, axis):
    return lax.broadcasted_iota(jnp.int32, shape, axis)


def dot(a, b):
    return jnp.dot(a, b, preferred_element_type=F32)


def hot(mask):
    return jnp.where(mask, 1.0, 0.0).astype(BF16)


def remote(src, dst, send, recv, keys, view):
    return pltpu.make_async_remote_copy(
        src_ref=src, dst_ref=dst, send_sem=send, recv_sem=recv,
        device_id=(keys, view), device_id_type=pl.DeviceIdType.MESH,
    )


def aligned(start, count):
    return pl.ds(pl.multiple_of(start, count), count)


def pack_plan(owners, keys_dev, cap, table_ref, key_ref, mult_ref, group_ref, count):
    key = as_row(key_ref)
    rows = key.shape[1]
    table = table_ref[...]
    tiles = table.shape[0]
    halves = jnp.concatenate([table & 255, table >> 8], axis=0).astype(F32).astype(BF16)
    looked = dot(halves, hot(iota((LANES, rows), 0) == (key & (LANES - 1))))
    high = iota((tiles, rows), 0) == (key >> 7)
    slot_low = jnp.sum(jnp.where(high, looked[:tiles], 0.0), axis=0, keepdims=True)
    slot_high = jnp.sum(jnp.where(high, looked[tiles:], 0.0), axis=0, keepdims=True)
    slot = slot_low.astype(jnp.int32) + 256 * slot_high.astype(jnp.int32)
    owner = slot // keys_dev
    local = slot - owner * keys_dev
    alive = iota((1, rows), 1) < count
    marks = jnp.where((iota((owners, rows), 0) == owner) & alive, 1.0, 0.0)
    step = min(256, rows)
    upper = hot(iota((step, step), 0) < iota((step, step), 1))
    running = jnp.zeros((owners, 1), F32)
    ranks = []
    for at in range(0, rows, step):
        piece = marks[:, at:at + step]
        before = dot(piece.astype(BF16), upper) + running
        ranks.append(jnp.sum(piece * before, axis=0, keepdims=True))
        running = running + jnp.sum(piece, axis=1, keepdims=True)
    rank = jnp.concatenate(ranks, axis=1).astype(jnp.int32)
    dest = jnp.where(alive, owner * cap + rank, -1)
    sign = as_row(mult_ref).astype(F32)
    parts = [local & 255, local >> 8]
    if group_ref is not None:
        group = as_row(group_ref)
        parts += [group & 255, group >> 8]
    meta = jnp.concatenate(
        [p.astype(F32) * sign for p in parts] + [jnp.zeros((META - len(parts), rows), F32)], axis=0
    ).astype(BF16)
    return dest, sign, meta


def packed(plan, cap, pay_ref, owner):
    dest, sign, meta = plan
    place = jnp.where(iota((cap, dest.shape[1]), 0) == dest - owner * cap, sign, 0.0).astype(BF16)
    columns = lax.dot_general(meta, place, (((1,), (1,)), ((), ())), preferred_element_type=F32)
    return dot(place, pay_ref[...]).astype(BF16), columns.astype(BF16)


def put_meta(ref, at, cap, columns):
    lanes = ref.shape[2]
    for t, lane in enumerate(range(0, cap, lanes)):
        wide = min(lanes, cap - lane)
        ref[at, cap + t * META:cap + (t + 1) * META, :wide] = columns[:, lane:lane + wide]


def meta_row(ref, at, row, cap):
    lanes = ref.shape[2]
    found = []
    for r in (row, row + 1):
        pieces = []
        for t, lane in enumerate(range(0, cap, lanes)):
            place = cap + t * META + r
            pieces.append(ref[at, place:place + 1, :min(lanes, cap - lane)].astype(F32))
        found.append(jnp.concatenate(pieces, axis=1).astype(jnp.int32))
    return found[0] + 256 * found[1]


def split(x):
    top = x.astype(BF16)
    return jnp.concatenate([top, (x - top.astype(F32)).astype(BF16)], axis=1)


def columns_of(row, width):
    return jnp.transpose(jnp.broadcast_to(row, (width, row.shape[1])))


def slot_marks(row, weight, keys_dev):
    count = row.shape[1]
    code = columns_of(row * 4 + weight, LANES)
    slot, scale = code >> 2, (code & 3).astype(F32)
    return jnp.concatenate(
        [
            jnp.where(iota((count, LANES), 1) + at == slot, scale, 0.0).astype(BF16)
            for at in range(0, keys_dev, LANES)
        ],
        axis=1,
    )


def kernel(d, *refs):
    da_count, db_count, *held_away, a_hbm, b_hbm, da_hbm, db_hbm, out = refs[:18]
    s = types.SimpleNamespace(**dict(zip(d.names, refs[18:], strict=True)))
    n, views, cap, slots, groups, width = d.owners, d.views, d.cap, d.slots, d.groups, d.width
    half, held = width // 2, d.held
    me, view = lax.axis_index("keys"), lax.axis_index("view")
    core = view & 1
    low = n // 2
    side = me // low
    place = me - side * low
    a_rows = s.a_pay.shape[0]

    groups_of = ((0, s.key_slot), (1, s.db_ints), (2, s.da_ints), (3, s.ab_ints))
    copies = []
    for i, to in groups_of:
        for r in range(to.shape[0]):
            copies.append(pltpu.make_async_copy(held_away[len(copies)], to.at[r], s.load.at[4 + i]))
    loads = [
        pltpu.make_async_copy(src, dst, s.load.at[i])
        for i, (src, dst) in enumerate(
            ((db_hbm, s.db_pay), (da_hbm, s.da_pay), (b_hbm, s.b_pay), (a_hbm, s.a_pay))
        )
    ]
    for load in copies[:3] + loads[:1] + copies[3:] + loads[1:]:
        load.start()

    def loaded(i):
        to = groups_of[i][1]
        pltpu.make_async_copy(to, to, s.load.at[4 + i]).wait()

    def sent(ref, semaphore):
        remote(ref, ref, semaphore, semaphore, me, view).wait_send()

    def landed(ref, semaphore):
        remote(ref, ref, semaphore, semaphore, me, view).wait_recv()

    barrier = pltpu.get_barrier_semaphore()
    devices = n * views
    mine = me * views + view

    def greet(i, carry):
        other = lax.rem(mine + i, devices)
        pl.semaphore_signal(
            barrier, inc=1, device_id=(other // views, lax.rem(other, views)),
            device_id_type=pl.DeviceIdType.MESH,
        )
        return carry

    lax.fori_loop(1, devices, greet, 0)

    loaded(0)
    loaded(1)
    b_plan = pack_plan(n, slots, cap, s.key_slot.at[0], s.db_ints.at[0], s.db_ints.at[1], None, db_count[0])
    loads[0].wait()

    from_me = core * low + place

    def row_copy(src, dst, send, recv, owner, source):
        there = owner // low
        return remote(
            src.at[owner], dst.at[source], send, recv,
            side * low + owner - there * low, (view - core) + there,
        )

    def b_copy(j, owner, source):
        src, dst = ((s.b_out0, s.b_in0), (s.b_out1, s.b_in1))[j]
        recv = s.b_recv.at[source] if j == 0 else s.b_later.at[source // low]
        return row_copy(src, dst, s.b_send.at[j], recv, owner, source)

    def d_copy(owner, source):
        return row_copy(s.d_out, s.d_in, s.d_send, s.d_recv.at[source], owner, source)

    def b_pack(low_ref, high_ref, at):
        rows, columns = packed(b_plan, cap, s.db_pay, at)
        low_ref[at, :cap, :] = rows[:, :half]
        high_ref[at, :cap, :] = rows[:, half:]
        put_meta(low_ref, at, cap, columns)

    def b_one(i, carry):
        b_pack(s.b_out0, s.b_out1, from_me ^ (n - i))
        return carry

    def b_start(j, i, carry):
        b_copy(j, from_me ^ (n - i), from_me).start()
        return carry

    def b_both(i, carry):
        b_one(i, carry)
        return b_start(0, i, carry)

    early = min(2, n)
    lax.fori_loop(1, early, b_one, 0)
    pl.semaphore_wait(barrier, devices - 1)
    lax.fori_loop(1, early, functools.partial(b_start, 0), 0)
    lax.fori_loop(early, n, b_both, 0)
    lax.fori_loop(1, n, functools.partial(b_start, 1), 0)
    b_pack(s.b_in0, s.b_in1, from_me)

    right = core == side
    wide = views // 2
    spot_x = view // 2
    piece = slots // wide
    own = aligned(spot_x * piece, piece)
    ahead = [(i - 1, lax.rem(spot_x + i, wide)) for i in range(1, wide)]
    behind = [(i - 1, lax.rem(spot_x + wide - i, wide)) for i in range(1, wide)]

    def wrong(run):
        pl.when(core != side)(run)

    base_pair = remote(s.base, s.base_first, s.pair_send, s.pair_recv, me, view ^ 1)

    def base_copy(i, p):
        at = aligned(p * piece, piece)
        return remote(s.base.at[at], s.base_in.at[i], s.base_send.at[i], s.base_recv.at[i], me, p * 2 + core)

    def base_add():
        @pl.when(right)
        def _():
            base_pair.wait_recv()
            s.base[...] += s.base_first[...]
            for i, p in ahead:
                base_copy(i, p).start()

    def base_end():
        @pl.when(right)
        def _():
            s.base_total[own, :] = s.base[own, :]
            for i, p in behind:
                base_copy(i, p).wait_recv()
                s.base_total[own, :] += s.base_in[i]

    def base_all(i, p, source):
        at = s.base_total.at[aligned(source * piece, piece)]
        return remote(at, at, s.all_send.at[i], s.all_recv.at[i], me, p * 2 + core)

    def base_spread():
        @pl.when(right)
        def _():
            for i, p in ahead:
                base_all(i, p, spot_x).start()

    sub = piece // 2
    subs = [pl.ds(q * sub, sub) for q in range(2)]

    def part_of(p, q):
        return aligned(p * piece + q * sub, sub)

    def wide_copy(j, i, p, q):
        return remote(
            s.part.at[j, part_of(p, q)], s.part_in.at[j, i, subs[q]], s.w_send, s.w_recv.at[j, i, q], me, p * 2 + core
        )

    def cross_copy(j, q):
        return remote(
            s.part_mid.at[j, subs[q]], s.part_first.at[j, subs[q]], s.x_send, s.x_recv.at[j, q], me ^ low, view
        )

    def total_copy(j, i, q):
        at = s.part_total.at[j, part_of(spot_x, q)]
        return remote(at, at, s.g_send.at[i - 1], s.g_recv.at[j, spot_x], me, lax.rem(view + i, views))

    def total_landed(j, p):
        landed(s.part_total.at[j, aligned(p * piece, piece)], s.g_recv.at[j, p])

    def table_copy(j):
        at = s.d_table.at[j, own, pl.ds(0, half)]
        return remote(at, at, s.c_send, s.c_recv.at[j], me ^ low, view)

    def table_peer(j, i, p, source):
        at = s.d_table.at[j, aligned(source * piece, piece), pl.ds(0, half)]
        return remote(at, at, s.t_send, s.t_recv.at[j, i], me, p * 2 + core)

    def wide_give(j):
        for q in range(2):
            for i, p in ahead:
                wide_copy(j, i, p, q).start()

    def wide_take(j):
        for q in range(2):
            total = s.part[j, part_of(spot_x, q)]
            for i, p in behind:
                wide_copy(j, i, p, q).wait_recv()
                total += s.part_in[j, i, subs[q]]
            s.part_mid[j, subs[q]] = total
            wrong(lambda: cross_copy(j, q).start())

    def total_give(j):
        @pl.when(right)
        def _():
            for q in range(2):
                cross_copy(j, q).wait_recv()
                s.part_total[j, part_of(spot_x, q)] = s.part_mid[j, subs[q]] + s.part_first[j, subs[q]]
                for i in range(1, views):
                    total_copy(j, i, q).start()
                if j == 1:
                    table_give(q)

    def table_give(j):
        s.d_table[j, own] = split(s.part_total[j, own] + s.base_total[own, j * half:(j + 1) * half])
        table_copy(j).start()

    def total_take(j):
        for _, p in behind:
            total_landed(j, p)
        wrong(lambda: total_landed(j, spot_x))

    def table_relay(j):
        @wrong
        def _():
            table_copy(j).wait_recv()
            for i, p in ahead:
                table_peer(j, i, p, spot_x).start()

    def table_take(j):
        @wrong
        def _():
            for i, p in behind:
                table_peer(j, i, p, p).wait_recv()

        @pl.when(right)
        def _():
            for _, p in behind:
                at = aligned(p * piece, piece)
                s.d_table[j, at] = split(s.part_total[j, at] + s.base_total[at, j * half:(j + 1) * half])

    loaded(3)
    loads[2].wait()
    chunk = min(1024, s.b_pay.shape[0])
    lines = chunk // LANES
    s.base[...] = jnp.zeros_like(s.base)

    def base_one(c, carry):
        slot = row_of(s.ab_ints.at[0], c * lines, lines)
        weight = row_of(s.ab_ints.at[1], c * lines, lines).astype(F32)
        marks = jnp.where(iota((slots, chunk), 0) == slot, weight, 0.0).astype(BF16)
        s.base[...] += dot(marks, s.b_pay[aligned(c * chunk, chunk), :])
        return carry

    lax.fori_loop(0, s.b_pay.shape[0] // chunk, base_one, 0)
    wrong(base_pair.start)

    few = min(512, a_rows)
    few_lines = few // LANES

    def slot_one(c, carry):
        s.a_marks[aligned(c * few, few), :] = slot_marks(
            row_of(s.ab_ints.at[2], c * few_lines, few_lines), row_of(s.ab_ints.at[3], c * few_lines, few_lines), slots
        )
        return carry

    loaded(2)
    d_plan = pack_plan(
        n, slots, cap, s.key_slot.at[0], s.da_ints.at[0], s.da_ints.at[2], s.da_ints.at[1], da_count[0]
    )
    loads[1].wait()
    def d_pack(ref, at, owner):
        rows, columns = packed(d_plan, cap, s.da_pay, owner)
        ref[at, :cap, :] = rows
        put_meta(ref, at, cap, columns)

    step_z = max(1, low // 2)

    def d_fill(i, carry):
        owner = from_me ^ i
        d_pack(s.d_out, owner, owner)
        return carry

    def d_start(i, carry):
        near = lax.rem(i, step_z)
        owner = from_me ^ ((i - near) * 2 + step_z + near)
        d_copy(owner, from_me).start()
        return carry

    def d_near(i, carry):
        near = lax.rem(i, step_z)
        owner = from_me ^ ((i - near) * 2 + near)
        d_copy(owner, from_me).start()
        return carry

    lax.fori_loop(1, n, d_fill, 0)
    lax.fori_loop(1, n // 2, d_near, 0)
    d_pack(s.d_in, from_me, from_me)

    @pl.when(core == side)
    def _():
        lax.fori_loop(0, n // 2, d_start, 0)

    block = min(256, groups // 2)
    blocks = groups // 2 // block
    span = min(2048, a_rows)
    span_lines = span // LANES

    def group_place(group):
        to = group // held
        turned = (to >> 1) ^ ((1 - side) * (devices // 4))
        return turned * held + group - to * held + jnp.where((to & 1) == core, groups // 2, 0)

    s.a_place[...] = group_place(s.ab_ints[4])

    def group_marks(g, count, at):
        return hot(iota((count, at.shape[1]), 0) + g * count == at)

    def a_group_marks(g, c):
        return group_marks(g, block, row_of(s.a_place, c * span_lines, span_lines))

    def a_groups():
        if not d.keep:
            return

        def one(g, carry):
            for c in range(a_rows // span):
                s.a_groups[aligned(g * block, block), c * span:(c + 1) * span] = a_group_marks(g, c)
            return carry

        lax.fori_loop(0, 2 * blocks, one, 0)

    def delta_sum(j):
        arrived_at = (s.b_in0, s.b_in1)[j]

        def fill(source):
            marks = hot(iota((slots, cap), 0) == meta_row(s.b_in0, source, 0, cap))
            if d.flat:
                s.b_marks[:, aligned(source * cap, cap)] = marks
            else:
                s.b_marks[source] = marks

        def step(i, carry):
            source = from_me ^ (n - i)
            b_copy(0, source, source).wait_recv()
            fill(source)
            return carry

        def gather(of):
            first = of * low
            rows = arrived_at[pl.ds(first, low), :cap, :].reshape(low * cap, half)
            if d.flat:
                return dot(s.b_marks[:, aligned(first * cap, low * cap)], rows)
            return lax.fori_loop(
                first, first + low, lambda i, total: total + dot(s.b_marks[i], arrived_at[i, :cap, :]),
                jnp.zeros((slots, half), F32),
            )

        if j == 0:
            lax.fori_loop(1, n - low + 1, step, 0)
        else:
            landed(s.b_in1.at[pl.ds(0, low)], s.b_later.at[1 - core])
        s.part[j] = gather(1 - core)
        if j == 0:
            fill(from_me)
            lax.fori_loop(n - low + 1, n, step, 0)
        else:
            landed(s.b_in1.at[pl.ds(0, low - 1)], s.b_later.at[core])
        s.part[j] += gather(core)

    def a_gather(j):
        s.a_table[...] = split(s.part_total[j])
        lanes = slice(j * half, (j + 1) * half)

        def step(c, carry):
            rows = aligned(c * span, span)
            both = dot(s.a_marks[rows, :], s.a_table[...])
            s.a_terms[rows, lanes] = (
                s.a_pay[rows, lanes].astype(F32) * (both[:, :half] + both[:, half:])
            ).astype(BF16)
            return carry

        lax.fori_loop(0, a_rows // span, step, 0, unroll=True)

    def d_arrive(first, last, far):
        def one(source):
            rows = aligned(source * cap, cap)
            s.d_marks[rows, :] = slot_marks(meta_row(s.d_in, source, 0, cap), jnp.ones((1, cap), jnp.int32), slots)
            if d.keep:
                s.d_groups[:, rows] = group_marks(0, groups, group_place(meta_row(s.d_in, source, 2, cap)))

        if first == 0 and not far:
            one(from_me)

        def step(i, carry):
            if far:
                i = lax.rem(i + jnp.where(core == side, 0, n // 4), n // 2)
            near = lax.rem(i, step_z)
            source = from_me ^ ((i - near) * 2 + near + (step_z if far else 0))
            d_copy(source, source).wait_recv()
            one(source)
            return carry

        lax.fori_loop(first if far else max(first, 1), last, step, 0)

    def a_sum(first, last):
        def step(g, carry):
            rows = aligned(g * block, block)
            if d.keep:
                s.view[rows, :] = dot(s.a_groups[rows, :], s.a_terms[...])
            else:
                s.view[rows, :] = sum(
                    dot(a_group_marks(g, c), s.a_terms[c * span:(c + 1) * span, :]) for c in range(a_rows // span)
                )
            return carry

        lax.fori_loop(first, last, step, 0, unroll=True)

    delta_sum(0)
    wide_give(0)
    lax.fori_loop(0, a_rows // few, slot_one, 0)

    delta_sum(1)
    wide_give(1)
    base_add()
    wide_take(0)
    a_groups()
    wide_take(1)
    @wrong
    def _():
        lax.fori_loop(0, n // 4, d_start, 0)

    total_give(0)
    @wrong
    def _():
        for j in range(2):
            s.d_table[j, :, half:] = jnp.zeros((slots, half), BF16)

    base_end()
    loads[3].wait()
    total_give(1)
    base_spread()
    d_arrive(0, n // 2, False)
    total_take(0)
    a_gather(0)
    @wrong
    def _():
        lax.fori_loop(n // 4, n // 2, d_start, 0)

    d_arrive(0, n // 4, True)
    total_take(1)
    a_gather(1)
    table_relay(0)
    a_sum(0, blocks)
    table_relay(1)
    a_sum(blocks, 2 * blocks)
    d_arrive(n // 4, n // 2, True)

    @pl.when(right)
    def _():
        for i, p in behind:
            base_all(i, p, p).wait_recv()

    several = min(n, span // cap)

    def d_gather(c, carry):
        rows = aligned(c * several * cap, several * cap)
        for j in range(2):
            lanes = slice(j * half, (j + 1) * half)
            both = dot(s.d_marks[rows, :], s.d_table[j])
            pay = s.d_in[pl.ds(c * several, several), :cap, lanes].reshape(several * cap, half)
            s.d_terms[rows, lanes] = (pay.astype(F32) * (both[:, :half] + both[:, half:])).astype(BF16)
        return carry

    table_take(0)
    table_take(1)
    lax.fori_loop(0, n // several, d_gather, 0)

    def d_sum(g):
        rows = aligned(g * block, block)
        if d.keep:
            return s.view[rows, :] + dot(s.d_groups[rows, :], s.d_terms[...])

        def one(source, total):
            marks = group_marks(g, block, group_place(meta_row(s.d_in, source, 2, cap)))
            return total + dot(marks, s.d_terms[aligned(source * cap, cap), :])

        return lax.fori_loop(0, n, one, s.view[rows, :])

    def pair_copy(g):
        rows = aligned(g * block, block)
        return remote(s.give.at[rows], s.take.at[rows], s.p_send, s.p_recv.at[g], me, view ^ 1)

    def give_one(g, carry):
        s.give[aligned(g * block, block), :] = d_sum(g)
        pair_copy(g).start()
        return carry

    lax.fori_loop(0, blocks, give_one, 0)
    pairs = views // 2
    spot = me * pairs + view // 2
    per = block // held

    def piece_copy(to, source):
        owner = to // pairs
        return remote(
            s.pieces.at[to], s.inbox.at[source], s.o_send, s.o_recv,
            owner, (to - owner * pairs) * 2 + core,
        )

    def keep_one(g, carry):
        total = d_sum(g + blocks)
        pair_copy(g).wait_recv()
        total = (total + s.take[aligned(g * block, block), :]).astype(BF16)
        for i in range(per):
            s.pieces[(g * per + i) ^ ((1 - side) * (devices // 4))] = total[i * held:(i + 1) * held, :]

        def send(i, inner):
            to = (g * per + i) ^ ((1 - side) * (devices // 4))

            @pl.when(to != spot)
            def _():
                piece_copy(to, spot).start()
            return inner

        lax.fori_loop(0, per, send, 0)
        return carry

    lax.fori_loop(0, blocks, keep_one, 0)
    everyone = n * pairs
    others = pl.ds(0, everyone - 1)
    s.inbox[spot] = s.pieces[spot]
    landed(s.inbox.at[others], s.o_recv)
    middle = everyone // 2
    out[0] = jnp.sum(s.inbox[:middle].astype(F32), axis=0)
    out[1] = jnp.sum(s.inbox[middle:].astype(F32), axis=0)

    rest = pl.ds(0, n - 1)
    sent(s.b_out0.at[rest], s.b_send.at[0])
    sent(s.b_out1.at[rest], s.b_send.at[1])
    sent(s.d_out.at[rest], s.d_send)
    sent(s.give, s.p_send)
    sent(s.pieces.at[others], s.o_send)
    sent(s.part.at[:, pl.ds(0, (wide - 1) * piece)], s.w_send)

    @wrong
    def _():
        base_pair.wait_send()
        sent(s.part_mid, s.x_send)
        sent(s.d_table.at[:, pl.ds(0, (wide - 1) * piece), pl.ds(0, half)], s.t_send)

    @pl.when(right)
    def _():
        for i, p in ahead:
            base_copy(i, p).wait_send()
            base_all(i, p, spot_x).wait_send()
        for i in range(views - 1):
            sent(s.part_mid, s.g_send.at[i])
        sent(s.d_table.at[:, own, pl.ds(0, half)], s.c_send)


def shards(
    groups, key_slot, a_slot, a_group, a_weight, a_payload, b_slot, b_weight, b_payload,
    da_key, da_group, da_mult, da_payload, da_count, db_key, db_mult, db_payload, db_count,
):
    owners, views = lax.axis_size("keys"), lax.axis_size("view")
    a_rows, width = a_payload.shape
    slots = key_slot.shape[0] // owners
    delta = da_payload.shape[0]
    cap = 2 * delta // owners
    half = width // 2
    held = groups // (owners * views)
    wide = views // 2
    piece = slots // wide
    block = min(256, groups // 2)
    blocks = groups // 2 // block
    flat = cap % LANES == 0
    keep = flat and 2 * groups * (a_rows + owners * cap) <= MARKS_LIMIT

    def lined(x):
        return x.reshape(-1, LANES)

    def tail(lanes):
        return max(2 * META, META * -(-cap // lanes))

    dma = pltpu.SemaphoreType.DMA
    ints = [
        lined(x)
        for x in (key_slot, db_key, db_mult, da_key, da_group, da_mult, b_slot, b_weight, a_slot, a_weight, a_group)
    ]
    scratch = dict(
        key_slot=pltpu.VMEM((1, *ints[0].shape), jnp.int32),
        db_ints=pltpu.VMEM((2, *ints[1].shape), jnp.int32),
        da_ints=pltpu.VMEM((3, *ints[3].shape), jnp.int32),
        ab_ints=pltpu.VMEM((5, *ints[6].shape), jnp.int32),
        a_pay=pltpu.VMEM(a_payload.shape, BF16),
        b_pay=pltpu.VMEM(b_payload.shape, BF16),
        da_pay=pltpu.VMEM(da_payload.shape, BF16),
        db_pay=pltpu.VMEM(db_payload.shape, BF16),
        b_out0=pltpu.VMEM((owners, cap + tail(half), half), BF16),
        b_out1=pltpu.VMEM((owners, cap, half), BF16),
        b_in0=pltpu.VMEM((owners, cap + tail(half), half), BF16),
        b_in1=pltpu.VMEM((owners, cap, half), BF16),
        d_out=pltpu.VMEM((owners, cap + tail(width), width), BF16),
        d_in=pltpu.VMEM((owners, cap + tail(width), width), BF16),
        b_marks=pltpu.VMEM((slots, owners * cap) if flat else (owners, slots, cap), BF16),
        a_marks=pltpu.VMEM((a_rows, slots), BF16),
        d_marks=pltpu.VMEM((owners * cap, slots), BF16),
        base=pltpu.VMEM((slots, width), F32),
        base_first=pltpu.VMEM((slots, width), F32),
        base_in=pltpu.VMEM((wide - 1, piece, width), F32),
        base_total=pltpu.VMEM((slots, width), F32),
        part=pltpu.VMEM((2, slots, half), F32),
        part_in=pltpu.VMEM((2, wide - 1, piece, half), F32),
        part_mid=pltpu.VMEM((2, piece, half), F32),
        part_first=pltpu.VMEM((2, piece, half), F32),
        part_total=pltpu.VMEM((2, slots, half), F32),
        a_table=pltpu.VMEM((slots, width), BF16),
        d_table=pltpu.VMEM((2, slots, width), BF16),
        a_terms=pltpu.VMEM((a_rows, width), BF16),
        d_terms=pltpu.VMEM((owners * cap, width), BF16),
        a_place=pltpu.VMEM((a_rows // LANES, LANES), jnp.int32),
        view=pltpu.VMEM((groups, width), F32),
        give=pltpu.VMEM((groups // 2, width), F32),
        take=pltpu.VMEM((groups // 2, width), F32),
        pieces=pltpu.VMEM((owners * views // 2, held, width), BF16),
        inbox=pltpu.VMEM((owners * views // 2, held, width), BF16),
        load=dma((8,)),
        b_send=dma((2,)),
        b_recv=dma((owners,)),
        b_later=dma((2,)),
        d_send=dma,
        d_recv=dma((owners,)),
        pair_send=dma,
        pair_recv=dma,
        base_send=dma((wide - 1,)),
        base_recv=dma((wide - 1,)),
        all_send=dma((wide - 1,)),
        all_recv=dma((wide - 1,)),
        w_send=dma,
        w_recv=dma((2, wide - 1, 2)),
        x_send=dma,
        x_recv=dma((2, 2)),
        g_send=dma((views - 1,)),
        g_recv=dma((2, wide)),
        c_send=dma,
        c_recv=dma((2,)),
        t_send=dma,
        t_recv=dma((2, wide - 1)),
        p_send=dma,
        p_recv=dma((blocks,)),
        o_send=dma,
        o_recv=dma,
    )
    if keep:
        scratch["a_groups"] = pltpu.VMEM((groups, a_rows), BF16)
        scratch["d_groups"] = pltpu.VMEM((groups, owners * cap), BF16)
    dims = types.SimpleNamespace(
        names=tuple(scratch), owners=owners, views=views, cap=cap, slots=slots, groups=groups, width=width,
        held=held, keep=keep, flat=flat,
    )
    vmem, smem = pl.BlockSpec(memory_space=pltpu.VMEM), pl.BlockSpec(memory_space=pltpu.SMEM)
    away = pl.BlockSpec(memory_space=pl.ANY)
    sums = pl.pallas_call(
        functools.partial(kernel, dims),
        out_shape=pltpu.VMEM((2, held, width), F32),
        in_specs=[smem] * 2 + [away] * 15,
        out_specs=vmem,
        scratch_shapes=list(scratch.values()),
        compiler_params=pltpu.CompilerParams(
            collective_id=0, has_side_effects=True, vmem_limit_bytes=VMEM_LIMIT
        ),
        name="delta_view",
    )(
        da_count, db_count, *ints,
        a_payload, b_payload, da_payload, db_payload,
    )
    return sums[0] + sums[1]


GROUPS_DEV = 32


def solution(mesh):
    row, wide = P(("keys", "view")), P(("keys", "view"), None)
    groups = GROUPS_DEV * mesh.shape["keys"] * mesh.shape["view"]
    in_specs = (P(), row, row, row, wide, row, row, wide, row, row, row, wide, row, row, row, wide, row)
    return jax.shard_map(
        functools.partial(shards, groups), mesh=mesh, in_specs=in_specs, out_specs=wide, check_vma=False
    )
```
